128 devices in a mesh: gx: 4 (over y_lo, core), gy: 4 (over z), gz: 8 (over y_hi, x).
Axes of the slice: x: 4, y: 4 (y_hi: 2, y_lo: 2; y = y_hi * 2 + y_lo), z: 4, core: 2. Of those that a mesh axis runs over, the one named last changes fastest.
Arguments:
- source: float32 [256, 256, 256], P('gx', 'gy', 'gz'), may hold values from -6 to 6
- green: float32 [512, 512, 512], P(None, ('gx', 'gz'), 'gy'), may hold values from 0.05 to 2, as said below
Outputs:
- potential: float32 [256, 256, 256], P('gx', 'gy', 'gz')
The draws below stay inside these ranges and needn't reach their ends.
Inputs may be any that keep to these rules, and one draw needn't show every extreme that they name: `green`: greenfull is even: greenfull[k] equals greenfull at (-k1 mod 512, -k2 mod 512, -k3 mod 512).
All inputs are finite; a program needn't handle non-finite values.
Results may differ from the reference program's by a relative error of at most 0.00007.
Values sent between devices are 32-bit elements; how exact they have to be, the bound alone decides.
A program may use at most 128 MiB of HBM per device.

```python
import math
import jax
import jax.numpy as jnp

NX = 256
NY = 256
NZ = 256
LX = 512
LY = 512
LZ = 512


def pair_frequency(length):
    position = jnp.arange(length, dtype=jnp.int32)
    unit_index = position // 2
    member = position % 2
    return jnp.where(unit_index == 0, member * (length // 2), jnp.where(member == 0, unit_index, length - unit_index)).astype(jnp.int32)


def draw_green(key, part):
    lower_end = 0.05
    upper_end = 2.0
    drawn = jnp.exp(jax.random.uniform(key, (LX, LY, LZ), jnp.float32, math.log(lower_end), math.log(upper_end)))
    mirrored = jnp.roll(jnp.flip(drawn, (0, 1, 2)), (1, 1, 1), (0, 1, 2))
    symmetric = 0.5 * (drawn + mirrored)
    ordered = jnp.take(symmetric, pair_frequency(LY), axis=1)
    return jnp.take(ordered, pair_frequency(LZ), axis=2)


def level_of(rng, shape, cuts, smallest, top_value):
    factor_of, own = 1.0, jax.random.fold_in(rng, 6)
    for axis_at, shards_of in cuts:
        heights = jnp.exp(jax.random.uniform(jax.random.fold_in(own, axis_at), (shards_of,), jnp.float32, smallest / len(cuts), top_value / len(cuts)))
        factor_of = factor_of * jnp.repeat(heights, shape[axis_at] // shards_of).reshape([-1 if axis == axis_at else 1 for axis in range(len(shape))])
    return factor_of


def centred(stream_key, shape, spread, bound, shards=(), kind=jnp.bfloat16):
    entries = spread * jax.random.normal(stream_key, shape, jnp.float32)
    if shards:
        entries = entries * level_of(stream_key, shape, shards, -0.22, 0.18)
    return jnp.clip(entries, -bound, bound).astype(kind)


def setup_inputs(seed: int = 0) -> dict:
    key_list = jax.random.split(jax.random.key(seed), 3)
    source = centred(key_list[0], (NX, NY, NZ), 1.0, 6.0, ((0, 4), (1, 4), (2, 8)), jnp.float32)
    green = draw_green(jax.random.fold_in(key_list[2], 71), 0)
    return {"source": source, "green": green}


def pair_position(length):
    freq = jnp.arange(length, dtype=jnp.int32)
    half = length // 2
    return jnp.where(freq == 0, 0, jnp.where(freq == half, 1, jnp.where(freq < half, 2 * freq, 2 * (length - freq) + 1))).astype(jnp.int32)


def reference(source, green):
    natural = jnp.take(green, pair_position(LY), axis=1)
    natural = jnp.take(natural, pair_position(LZ), axis=2)
    padded = jnp.pad(source, ((0, NX), (0, NY), (0, NZ)))
    spectrum = jnp.fft.fftn(padded)
    inverse = jnp.fft.ifftn(spectrum * natural)
    return jnp.real(inverse)[:NX, :NY, :NZ].astype(jnp.float32)
```

```python
import functools

import jax
import jax.numpy as jnp
import numpy as np
from jax import lax
from jax.experimental import pallas as pl
from jax.experimental.pallas import tpu as pltpu
from jax.sharding import PartitionSpec as P

MESH = pl.DeviceIdType.MESH
F32 = jnp.float32
BF16 = jnp.bfloat16
GX, GY, GZ = 4, 4, 8
GROUP = GY * GZ
ALL = GX * GROUP


def halves(table):
    high = np.asarray(table, np.float32).astype(BF16)
    low = (np.asarray(table) - high.astype(np.float64)).astype(np.float32).astype(BF16)
    return np.stack([high, low])


def tables():
    n = np.arange(256)
    angle = 2.0 * np.pi * ((n[:, None] * n[None, :]) % 512) / 512.0
    parity = 1.0 - 2.0 * (n % 2)
    cos, sin = np.cos(angle), np.sin(angle)
    sin_rows = sin.copy()
    sin_rows[0, :] = parity
    sin_cols = sin.copy()
    sin_cols[:, 0] = parity
    lines = np.concatenate([halves(cos), halves(sin_rows), halves(sin_cols)])
    real = cos.reshape(256, 4, 1, 64)
    imag = -sin
    imag[:, 0] = parity
    forward = np.concatenate([real, imag.reshape(256, 4, 1, 64)], axis=2)
    weight = np.full((4, 2, 64), 2.0)
    weight[0, :, 0] = 1.0
    inverse = (forward * weight[None]).reshape(256, 512).T
    return lines, halves(forward.reshape(256, 512)), halves(inverse)


def split(value):
    high = value.astype(BF16)
    return high, (value - high.astype(F32)).astype(BF16)


def dot(left, right):
    return jnp.dot(left, right, preferred_element_type=F32)


def dot3(left, right):
    return dot(left[0], right[0]) + (dot(left[1], right[0]) + dot(left[0], right[1]))


def kernel(src_hbm, green_hbm, lines_hbm, zf_hbm, zi_hbm, out_ref,
           src, lines, zf, zi, got1, zs, zb, snd, rcv, back, gbuf, gs, gmix, snd4, got4,
           in_sem, tab_sem, green_sem, s1, r1, s2, r2, s3, r3, s4, r4):
    a, b, c = lax.axis_index("gx"), lax.axis_index("gy"), lax.axis_index("gz")
    q = b * GZ + c
    me = a * GROUP + q

    load_src = pltpu.make_async_copy(src_hbm, src, in_sem)
    load_src.start()
    loads = [pltpu.make_async_copy(lines_hbm, lines, tab_sem.at[0]),
             pltpu.make_async_copy(zf_hbm, zf, tab_sem.at[1]),
             pltpu.make_async_copy(zi_hbm, zi, tab_sem.at[2])]
    for load in loads:
        load.start()

    def group_peer(o):
        pb = lax.rem(b + o // GZ, GY)
        pc = lax.rem(c + lax.rem(o, GZ), GZ)
        return pb, pc

    def any_peer(o):
        pa = lax.rem(a + o // GROUP, GX)
        pb, pc = group_peer(lax.rem(o, GROUP))
        return pa, pb, pc

    bar = pltpu.get_barrier_semaphore()

    def greet(o, carry):
        pa, pb, pc = any_peer(o)
        pl.semaphore_signal(bar, inc=1, device_id=(pa, pb, pc), device_id_type=MESH)
        return carry

    lax.fori_loop(1, ALL, greet, 0)
    pl.semaphore_wait(bar, ALL - 1)
    load_src.wait()

    def send1(o, carry):
        pb, pc = group_peer(o)
        pltpu.make_async_remote_copy(
            src.at[pb * GZ + pc], got1.at[q], s1, r1, device_id=(a, pb, pc), device_id_type=MESH
        ).start()
        return carry

    lax.fori_loop(1, GROUP, send1, 0)
    got1[q] = src[q]

    pltpu.make_async_copy(green_hbm.at[pl.ds(0, 257)], gbuf.at[pl.ds(0, 257)], green_sem).start()

    def load_green(k, carry):
        pltpu.make_async_copy(green_hbm.at[512 - k], gbuf.at[256 + k], green_sem).start()
        return carry

    lax.fori_loop(1, 256, load_green, 0)
    for load in loads:
        load.wait()
    def wait_bytes(part, sem):
        pltpu.make_async_copy(part, part, sem).wait()

    wait_bytes(got1.at[pl.ds(0, GROUP - 1)], r1)

    lane = lax.broadcasted_iota(jnp.int32, (16, 128), 1) // 32

    for i in range(2):
        def gather(t, carry):
            tb, th = t // 2, lax.rem(t, 2)
            pieces = [got1[tb * GZ + th * 4 + m, i] for m in range(4)]
            for yh in range(4):
                tile = pieces[0] if yh == 0 else pltpu.roll(pieces[0], (-yh * 32) % 128, 1)
                for m in range(1, 4):
                    shift = ((m - yh) * 32) % 128
                    moved = pieces[m] if shift == 0 else pltpu.roll(pieces[m], shift, 1)
                    tile = jnp.where(lane == m, moved, tile)
                row = pl.multiple_of(tb * 64 + yh * 16, 16)
                zs[th, i, pl.ds(row, 16), :] = tile
            return carry

        lax.fori_loop(0, 8, gather, 0)

    sign = jnp.where(lax.broadcasted_iota(jnp.int32, (1, 128), 1) < 64, 1.0, -1.0).astype(F32)
    real_lane = lax.broadcasted_iota(jnp.int32, (1, 128), 1) == 0
    imag_lane = lax.broadcasted_iota(jnp.int32, (1, 128), 1) == 64
    unit_lane = jnp.logical_or(real_lane, imag_lane)
    top_row = lax.broadcasted_iota(jnp.int32, (8, 1), 0) == 0

    def turn(value):
        return sign * pltpu.roll(value, 64, 1)

    def fix_top(value, top):
        return jnp.concatenate([jnp.where(top_row, top, value[:8]), value[8:]], axis=0)

    cos = (lines[0], lines[1])
    sin_rows = (lines[2], lines[3])
    sin_cols = (lines[4], lines[5])

    for i in range(2):
        rows = jnp.concatenate([zs[0, i], zs[1, i]], axis=1)
        zb[i] = dot3(split(rows), (zf[0], zf[1]))

    snd_view = snd.reshape(2, GX, GY, GZ, 2, 8, 128)

    def forward_y(t, carry):
        i, tb = t // GY, lax.rem(t, GY)
        column = pl.multiple_of(tb * 128, 128)
        value = zb[i, :, pl.ds(column, 128)]
        even = dot3(cos, split(value))
        odd = dot3(sin_rows, split(turn(value)))
        plus, minus = even + odd, even - odd
        special = jnp.logical_and(unit_lane, tb == 0)
        even_turn, odd_turn = pltpu.roll(even, 64, 1), pltpu.roll(odd, 64, 1)
        plus = jnp.where(special, jnp.where(real_lane, even, odd), plus)
        minus = jnp.where(special, jnp.where(real_lane, even_turn, -odd_turn), minus)
        plus = fix_top(plus, even[:8])
        minus = fix_top(minus, -sign * odd_turn[:8])
        snd_view[0, :, tb, :, i] = plus.reshape(GX, GZ, 8, 128)
        snd_view[1, :, tb, :, i] = minus.reshape(GX, GZ, 8, 128)
        return carry

    lax.fori_loop(0, 2 * GY, forward_y, 0)

    for s in range(2):
        def send2(o, carry):
            pa, pb, pc = any_peer(o)
            pltpu.make_async_remote_copy(
                snd.at[s, pa * GROUP + pb * GZ + pc], rcv.at[s, pl.ds(2 * me, 2)], s2.at[s], r2.at[s],
                device_id=(pa, pb, pc), device_id_type=MESH
            ).start()
            return carry

        lax.fori_loop(1, ALL, send2, 0)
        rcv[s, pl.ds(2 * me, 2)] = snd[s, me]

    pltpu.make_async_copy(green_hbm, gbuf, green_sem).wait()
    green_rows = gbuf.reshape(512 * 16, 128)
    corner = jnp.logical_and(b == 0, jnp.logical_and(a == 0, c == 0))
    pick = 2 * lax.rem(lax.broadcasted_iota(jnp.int32, (512, 128), 1), 64)

    def prepare(jj, carry):
        first = green_rows[pl.ds(2 * jj, 512, stride=16), :]
        second = green_rows[pl.ds(2 * jj + 1, 512, stride=16), :]
        here = jnp.logical_and(corner, jj == 0)
        plus = jnp.take_along_axis(first, pick, axis=1)
        minus = jnp.take_along_axis(second, pick, axis=1)
        first0, first1 = first[:, 0:1], first[:, 1:2]
        second0, second1 = second[:, 0:1], second[:, 1:2]
        at_unit = jnp.logical_and(unit_lane, b == 0)
        plus_unit = jnp.where(here, 0.5 * (first0 + first1), first0)
        minus_unit = jnp.where(here, 0.5 * (second0 + second1), first1)
        gs[0, jj] = jnp.where(at_unit, plus_unit, plus)
        gs[1, jj] = jnp.where(at_unit, minus_unit, minus)

        @pl.when(jj == 0)
        def _():
            gmix[0] = jnp.where(jnp.logical_and(unit_lane, here), 0.5 * (first0 - first1), 0.0)
            gmix[1] = jnp.where(jnp.logical_and(unit_lane, here), 0.5 * (second0 - second1), 0.0)

        return carry

    lax.fori_loop(0, 8, prepare, 0)

    def wide(left, right):
        return jnp.concatenate([left, right], axis=1)

    rcv_rows = rcv.reshape(2 * 256 * 8, 128)
    for s in range(2):
        wait_bytes(rcv.at[s, pl.ds(0, 2 * (ALL - 1))], r2.at[s])

        def lines_x(jp, carry):
            first = pl.ds(s * 2048 + 2 * jp, 256, stride=8)
            second = pl.ds(s * 2048 + 2 * jp + 1, 256, stride=8)
            left, right = rcv_rows[first, :], rcv_rows[second, :]
            even = dot3(cos, split(wide(left, right)))
            odd = dot3(sin_rows, split(wide(turn(left), turn(right))))
            results = []
            for h in range(2):
                ev, od = even[:, h * 128:(h + 1) * 128], odd[:, h * 128:(h + 1) * 128]
                plus = fix_top(ev + od, ev[:8])
                minus = fix_top(ev - od, -turn(od[:8]))
                out_plus = plus * gs[s, 2 * jp + h, 0:256]
                out_minus = minus * gs[s, 2 * jp + h, 256:512]
                if h == 0:
                    mix = jnp.where(jp == 0, 1.0, 0.0) * sign
                    out_plus += gmix[s, 0:256] * (mix * fix_top(minus, plus[:8]))
                    out_minus += gmix[s, 256:512] * (mix * fix_top(plus, minus[:8]))
                total = fix_top(out_plus + out_minus, out_plus[:8])
                turned = fix_top(turn(out_plus - out_minus), -out_minus[:8])
                results.append((total, turned))
            total = wide(results[0][0], results[1][0])
            turned = wide(results[0][1], results[1][1])
            back_x = dot3(cos, split(total)) - dot3(sin_cols, split(turned))
            rcv_rows[first, :] = back_x[:, :128]
            rcv_rows[second, :] = back_x[:, 128:]
            return carry

        lax.fori_loop(0, 4, lines_x, 0)

        def send3(o, carry):
            pa, pb, pc = any_peer(o)
            peer = pa * GROUP + pb * GZ + pc
            pltpu.make_async_remote_copy(
                rcv.at[s, pl.ds(2 * peer, 2)], back.at[s, me], s3.at[s], r3.at[s],
                device_id=(pa, pb, pc), device_id_type=MESH
            ).start()
            return carry

        lax.fori_loop(1, ALL, send3, 0)
        back[s, me] = rcv[s, pl.ds(2 * me, 2)]

    for s in range(2):
        wait_bytes(back.at[s, pl.ds(0, ALL - 1)], r3.at[s])

    back_view = back.reshape(2, GX, GY, GZ, 2, 8, 128)

    def inverse_y(t, carry):
        i, tb = t // GY, lax.rem(t, GY)
        plus = back_view[0, :, tb, :, i].reshape(256, 128)
        minus = back_view[1, :, tb, :, i].reshape(256, 128)
        special = jnp.logical_and(unit_lane, tb == 0)
        total = plus + minus
        turned = turn(plus - minus)
        total = jnp.where(special, 2.0 * jnp.where(real_lane, plus, pltpu.roll(minus, 64, 1)), total)
        turned = jnp.where(special, 2.0 * jnp.where(real_lane, pltpu.roll(plus, 64, 1), minus), turned)
        total = fix_top(total, plus[:8])
        turned = fix_top(turned, -minus[:8])
        column = pl.multiple_of(tb * 128, 128)
        zb[i, :, pl.ds(column, 128)] = dot3(cos, split(total)) - dot3(sin_cols, split(turned))
        return carry

    lax.fori_loop(0, 2 * GY, inverse_y, 0)

    for i in range(2):
        rows = dot3(split(zb[i]), (zi[0], zi[1])) * (1.0 / 134217728.0)
        zs[0, i] = rows[:, :128]
        zs[1, i] = rows[:, 128:]

    for i in range(2):
        def scatter(t, carry):
            tb, th = t // 2, lax.rem(t, 2)
            pieces = []
            for yh in range(4):
                row = pl.multiple_of(tb * 64 + yh * 16, 16)
                pieces.append(zs[th, i, pl.ds(row, 16), :])
            for m in range(4):
                tile = pieces[0] if m == 0 else pltpu.roll(pieces[0], (-m * 32) % 128, 1)
                for yh in range(1, 4):
                    shift = ((yh - m) * 32) % 128
                    moved = pieces[yh] if shift == 0 else pltpu.roll(pieces[yh], shift, 1)
                    tile = jnp.where(lane == yh, moved, tile)
                snd4[tb * GZ + th * 4 + m, i] = tile
            return carry

        lax.fori_loop(0, 8, scatter, 0)

    def send4(o, carry):
        pb, pc = group_peer(o)
        pltpu.make_async_remote_copy(
            snd4.at[pb * GZ + pc], got4.at[q], s4, r4, device_id=(a, pb, pc), device_id_type=MESH
        ).start()
        return carry

    lax.fori_loop(1, GROUP, send4, 0)
    got4[q] = snd4[q]
    for s in range(2):
        wait_bytes(snd.at[s, pl.ds(0, ALL - 1)], s2.at[s])
        wait_bytes(rcv.at[s, pl.ds(0, 2 * (ALL - 1))], s3.at[s])
    for ref, sem in ((src, s1), (got4, r4), (snd4, s4)):
        wait_bytes(ref.at[pl.ds(0, GROUP - 1)], sem)
    out_ref[...] = got4[...]


def per_device(source, green):
    lines, forward, inverse = tables()
    packed = source.reshape(64, 4, 16, 32).transpose(0, 2, 1, 3).reshape(GROUP, 2, 16, 128)
    vmem = pltpu.VMEM
    dma = pltpu.SemaphoreType.DMA
    result = pl.pallas_call(
        kernel,
        out_shape=jax.ShapeDtypeStruct((GROUP, 2, 16, 128), F32),
        in_specs=[pl.BlockSpec(memory_space=pl.ANY)] * 5,
        out_specs=pl.BlockSpec(memory_space=vmem),
        scratch_shapes=[
            vmem((GROUP, 2, 16, 128), F32),
            vmem((6, 256, 256), BF16),
            vmem((2, 256, 512), BF16),
            vmem((2, 512, 256), BF16),
            vmem((GROUP, 2, 16, 128), F32),
            vmem((2, 2, 256, 128), F32),
            vmem((2, 256, 512), F32),
            vmem((2, ALL, 2, 8, 128), F32),
            vmem((2, 256, 8, 128), F32),
            vmem((2, ALL, 2, 8, 128), F32),
            vmem((512, 16, 128), F32),
            vmem((2, 8, 512, 128), F32),
            vmem((2, 512, 128), F32),
            vmem((GROUP, 2, 16, 128), F32),
            vmem((GROUP, 2, 16, 128), F32),
            dma, dma((3,)), dma, dma, dma, dma((2,)), dma((2,)), dma((2,)), dma((2,)), dma, dma,
        ],
        compiler_params=pltpu.CompilerParams(
            collective_id=1, has_side_effects=True, vmem_limit_bytes=56 * 2**20
        ),
        name="poisson",
    )(packed, green, jnp.asarray(lines), jnp.asarray(forward), jnp.asarray(inverse))
    return result.reshape(64, 16, 4, 32).transpose(0, 2, 1, 3).reshape(64, 64, 32)


def solution(mesh):
    return jax.shard_map(
        per_device,
        mesh=mesh,
        in_specs=(P("gx", "gy", "gz"), P(None, ("gx", "gz"), "gy")),
        out_specs=P("gx", "gy", "gz"),
        check_vma=False,
    )
```

```python
import jax
import jax.numpy as jnp
import numpy as np
from jax import lax
from jax.experimental import pallas as pl
from jax.experimental.pallas import tpu as pltpu
from jax.sharding import PartitionSpec as P

FLAT = pl.DeviceIdType.LOGICAL
F32 = jnp.float32
BF16 = jnp.bfloat16
GX, GY, GZ = 4, 4, 8
GROUP = GY * GZ
ALL = GX * GROUP


def halves(table):
    high = np.asarray(table, np.float32).astype(BF16)
    low = (np.asarray(table) - high.astype(np.float64)).astype(np.float32).astype(BF16)
    return np.stack([high, low])


def tables():
    n = np.arange(256)
    angle = 2.0 * np.pi * ((n[:, None] * n[None, :]) % 512) / 512.0
    parity = 1.0 - 2.0 * (n % 2)
    cos, sin = np.cos(angle), np.sin(angle)
    sin_rows = sin.copy()
    sin_rows[0, :] = parity
    sin_cols = sin.copy()
    sin_cols[:, 0] = parity
    lines = np.concatenate([halves(cos), halves(sin_rows), halves(sin_cols)])
    real = cos.reshape(256, 4, 1, 64)
    imag = -sin
    imag[:, 0] = parity
    forward = np.concatenate([real, imag.reshape(256, 4, 1, 64)], axis=2)
    weight = np.full((4, 2, 64), 2.0)
    weight[0, :, 0] = 1.0
    inverse = (forward * weight[None]).reshape(256, 512)
    return lines, halves(forward.reshape(256, 512)), halves(inverse)


def split(value):
    high = value.astype(BF16)
    return high, (value - high.astype(F32)).astype(BF16)


def dot(left, right):
    return jnp.dot(left, right, preferred_element_type=F32)


def dot_t(left, right):
    return lax.dot_general(left, right, (((1,), (1,)), ((), ())), preferred_element_type=F32)


def dot3(left, right):
    return dot(left[0], right[0]) + (dot(left[1], right[0]) + dot(left[0], right[1]))


def wide(left, right):
    return jnp.concatenate([left, right], axis=1)


def kernel(src_hbm, green_hbm, lines_hbm, zf_hbm, zi_hbm, out_ref,
           src, pack, lines, zf, zi, got1, zs, zb, snd, rcv, back0, back1, gbuf, gs, gmix, snd4, got4,
           in_sem, tab_sem, green_sem, s1, r1, s2, r2, s30, r30, s31, r31, s4, r4):
    a, b, c = lax.axis_index("gx"), lax.axis_index("gy"), lax.axis_index("gz")
    q = b * GZ + c
    me = a * GROUP + q

    load_src = pltpu.make_async_copy(src_hbm, src, in_sem)
    load_src.start()
    loads = [pltpu.make_async_copy(lines_hbm, lines, tab_sem.at[0]),
             pltpu.make_async_copy(zf_hbm, zf, tab_sem.at[1]),
             pltpu.make_async_copy(zi_hbm, zi, tab_sem.at[2])]
    for load in loads:
        load.start()

    def wait_bytes(part, sem):
        pltpu.make_async_copy(part, part, sem).wait()

    def each_peer(count, body):
        def step(o, carry):
            body(lax.bitwise_xor(me, o))
            return carry

        lax.fori_loop(1, count, step, 0, unroll=8)

    bar = pltpu.get_barrier_semaphore()

    def greet(peer):
        pl.semaphore_signal(bar, inc=1, device_id=peer, device_id_type=FLAT)

    each_peer(GROUP, greet)
    for o in range(1, GX):
        greet(lax.bitwise_xor(me, o * GROUP))
    load_src.wait()

    def pack_x(p, carry):
        for i in range(2):
            plane = src[2 * p + i]
            pack[i, p] = wide(plane[:16], plane[16:])
        return carry

    lax.fori_loop(0, GROUP, pack_x, 0, unroll=4)
    pl.semaphore_wait(bar, GROUP - 1 + GX - 1)

    for i in range(2):
        def send1(peer):
            pltpu.make_async_remote_copy(
                pack.at[i, lax.rem(peer, GROUP)], got1.at[i, q], s1.at[i], r1.at[i],
                device_id=peer, device_id_type=FLAT
            ).start()

        each_peer(GROUP, send1)
        got1[i, q] = pack[i, q]

    pltpu.make_async_copy(green_hbm.at[pl.ds(0, 257)], gbuf.at[pl.ds(0, 257)], green_sem).start()

    def load_green(k, carry):
        pltpu.make_async_copy(green_hbm.at[512 - k], gbuf.at[256 + k], green_sem).start()
        return carry

    lax.fori_loop(1, 256, load_green, 0, unroll=5)
    for load in loads:
        load.wait()

    low_lane = lax.broadcasted_iota(jnp.int32, (1, 128), 1) < 64
    sign = jnp.where(low_lane, 1.0, -1.0).astype(F32)
    real_lane = lax.broadcasted_iota(jnp.int32, (1, 128), 1) == 0
    imag_lane = lax.broadcasted_iota(jnp.int32, (1, 128), 1) == 64
    unit_lane = jnp.logical_or(real_lane, imag_lane)
    top_row = lax.broadcasted_iota(jnp.int32, (8, 1), 0) == 0

    def half_turn(value):
        return pltpu.roll(value, 64, 1)

    def turn(value):
        return sign * half_turn(value)

    def fix_top(value, top):
        return jnp.concatenate([jnp.where(top_row, top, value[:8]), value[8:]], axis=0)

    cos = (lines[0], lines[1])
    sin_rows = (lines[2], lines[3])
    sin_cols = (lines[4], lines[5])
    snd_view = snd.reshape(2, 2, GX, GY, GZ, 8, 128)

    def send2(s, i):
        def send(peer):
            pltpu.make_async_remote_copy(
                snd.at[s, i, peer], rcv.at[s, 2 * me + i], s2.at[s], r2.at[s],
                device_id=peer, device_id_type=FLAT
            ).start()

        each_peer(ALL, send)
        rcv[s, 2 * me + i] = snd[s, i, me]

    for i in range(2):
        wait_bytes(got1.at[i, pl.ds(0, GROUP - 1)], r1.at[i])

        def gather(t, carry):
            for th in range(2):
                left = got1[i, 2 * th * GZ + t]
                right = got1[i, (2 * th + 1) * GZ + t]
                row = pl.multiple_of(t * 32, 32)
                zs[pl.ds(row, 16), th * 128:(th + 1) * 128] = jnp.where(low_lane, left, half_turn(right))
                zs[pl.ds(row + 16, 16), th * 128:(th + 1) * 128] = jnp.where(low_lane, half_turn(left), right)
            return carry

        lax.fori_loop(0, GZ, gather, 0, unroll=2)
        zb[...] = dot3(split(jnp.transpose(zs[...])), (zf[0], zf[1]))

        def forward_y(t, carry):
            column = pl.multiple_of(t * 256, 256)
            value = zb[:, pl.ds(column, 256)]
            even = dot3(cos, split(value))
            odd = dot3(sin_rows, split(wide(turn(value[:, :128]), turn(value[:, 128:]))))
            for h in range(2):
                ev, od = even[:, h * 128:(h + 1) * 128], odd[:, h * 128:(h + 1) * 128]
                plus, minus = ev + od, ev - od
                if h == 0:
                    special = jnp.logical_and(unit_lane, t == 0)
                    plus = jnp.where(special, jnp.where(real_lane, ev, od), plus)
                    minus = jnp.where(special, jnp.where(real_lane, half_turn(ev), -half_turn(od)), minus)
                plus = fix_top(plus, ev[:8])
                minus = fix_top(minus, -turn(od[:8]))
                snd_view[0, i, :, 2 * t + h] = plus.reshape(GX, GZ, 8, 128)
                snd_view[1, i, :, 2 * t + h] = minus.reshape(GX, GZ, 8, 128)
            return carry

        lax.fori_loop(0, GY // 2, forward_y, 0)
        send2(0, i)
    for i in range(2):
        send2(1, i)

    pltpu.make_async_copy(green_hbm, gbuf, green_sem).wait()
    green_rows = gbuf.reshape(512 * 16, 128)
    corner = jnp.logical_and(b == 0, jnp.logical_and(a == 0, c == 0))
    pick = 2 * lax.rem(lax.broadcasted_iota(jnp.int32, (512, 128), 1), 64)

    def prepare(jj, carry):
        first = green_rows[pl.ds(2 * jj, 512, stride=16), :]
        second = green_rows[pl.ds(2 * jj + 1, 512, stride=16), :]
        here = jnp.logical_and(corner, jj == 0)
        plus = jnp.take_along_axis(first, pick, axis=1)
        minus = jnp.take_along_axis(second, pick, axis=1)
        first0, first1 = first[:, 0:1], first[:, 1:2]
        second0, second1 = second[:, 0:1], second[:, 1:2]
        at_unit = jnp.logical_and(unit_lane, b == 0)
        plus_unit = jnp.where(here, 0.5 * (first0 + first1), first0)
        minus_unit = jnp.where(here, 0.5 * (second0 + second1), first1)
        gs[0, jj] = jnp.where(at_unit, plus_unit, plus)
        gs[1, jj] = jnp.where(at_unit, minus_unit, minus)

        @pl.when(jj == 0)
        def _():
            gmix[0] = jnp.where(jnp.logical_and(unit_lane, here), 0.5 * (first0 - first1), 0.0)
            gmix[1] = jnp.where(jnp.logical_and(unit_lane, here), 0.5 * (second0 - second1), 0.0)

        return carry

    lax.fori_loop(0, 8, prepare, 0)

    rcv_rows = rcv.reshape(2 * 256 * 8, 128)
    for s in range(2):
        wait_bytes(rcv.at[s, pl.ds(0, 2 * (ALL - 1))], r2.at[s])

        def lines_x(jp, carry):
            first = pl.ds(s * 2048 + 2 * jp, 256, stride=8)
            second = pl.ds(s * 2048 + 2 * jp + 1, 256, stride=8)
            left, right = rcv_rows[first, :], rcv_rows[second, :]
            even = dot3(cos, split(wide(left, right)))
            odd = dot3(sin_rows, split(wide(turn(left), turn(right))))
            results = []
            for h in range(2):
                ev, od = even[:, h * 128:(h + 1) * 128], odd[:, h * 128:(h + 1) * 128]
                plus = fix_top(ev + od, ev[:8])
                minus = fix_top(ev - od, -turn(od[:8]))
                out_plus = plus * gs[s, 2 * jp + h, 0:256]
                out_minus = minus * gs[s, 2 * jp + h, 256:512]
                if h == 0:
                    mix = jnp.where(jp == 0, 1.0, 0.0) * sign
                    out_plus += gmix[s, 0:256] * (mix * fix_top(minus, plus[:8]))
                    out_minus += gmix[s, 256:512] * (mix * fix_top(plus, minus[:8]))
                total = fix_top(out_plus + out_minus, out_plus[:8])
                turned = fix_top(turn(out_plus - out_minus), -out_minus[:8])
                results.append((total, turned))
            total = wide(results[0][0], results[1][0])
            turned = wide(results[0][1], results[1][1])
            back_x = dot3(cos, split(total)) - dot3(sin_cols, split(turned))
            rcv_rows[first, :] = back_x[:, :128]
            rcv_rows[second, :] = back_x[:, 128:]
            return carry

        lax.fori_loop(0, 4, lines_x, 0)

        if s == 0:
            def send30(peer):
                pltpu.make_async_remote_copy(
                    rcv.at[0, pl.ds(2 * peer, 2)], back0.at[me], s30, r30,
                    device_id=peer, device_id_type=FLAT
                ).start()

            each_peer(ALL, send30)
            back0[me] = rcv[0, pl.ds(2 * me, 2)]
        else:
            for i in range(2):
                def send31(peer):
                    pltpu.make_async_remote_copy(
                        rcv.at[1, 2 * peer + i], back1.at[i, me], s31.at[i], r31.at[i],
                        device_id=peer, device_id_type=FLAT
                    ).start()

                each_peer(ALL, send31)
                back1[i, me] = rcv[1, 2 * me + i]

    back0_view = back0.reshape(GX, GY, GZ, 2, 8, 128)
    back1_view = back1.reshape(2, GX, GY, GZ, 8, 128)
    wait_bytes(back0.at[pl.ds(0, ALL - 1)], r30)
    for i in range(2):
        wait_bytes(back1.at[i, pl.ds(0, ALL - 1)], r31.at[i])

        def inverse_y(t, carry):
            totals, turneds = [], []
            for h in range(2):
                plus = back0_view[:, 2 * t + h, :, i].reshape(256, 128)
                minus = back1_view[i, :, 2 * t + h].reshape(256, 128)
                total = plus + minus
                turned = turn(plus - minus)
                if h == 0:
                    special = jnp.logical_and(unit_lane, t == 0)
                    total = jnp.where(special, 2.0 * jnp.where(real_lane, plus, half_turn(minus)), total)
                    turned = jnp.where(special, 2.0 * jnp.where(real_lane, half_turn(plus), minus), turned)
                totals.append(fix_top(total, plus[:8]))
                turneds.append(fix_top(turned, -minus[:8]))
            column = pl.multiple_of(t * 256, 256)
            zb[:, pl.ds(column, 256)] = (
                dot3(cos, split(wide(*totals))) - dot3(sin_cols, split(wide(*turneds)))
            )
            return carry

        lax.fori_loop(0, GY // 2, inverse_y, 0)
        high, low = split(zb[...])
        zs[...] = (dot_t(zi[0], high) + (dot_t(zi[1], high) + dot_t(zi[0], low))) * (1.0 / 134217728.0)

        def scatter(t, carry):
            row = pl.multiple_of(t * 32, 32)
            for th in range(2):
                upper = zs[pl.ds(row, 16), th * 128:(th + 1) * 128]
                lower = zs[pl.ds(row + 16, 16), th * 128:(th + 1) * 128]
                snd4[i, 2 * th * GZ + t] = jnp.where(low_lane, upper, half_turn(lower))
                snd4[i, (2 * th + 1) * GZ + t] = jnp.where(low_lane, half_turn(upper), lower)
            return carry

        lax.fori_loop(0, GZ, scatter, 0, unroll=2)

        def send4(peer):
            pltpu.make_async_remote_copy(
                snd4.at[i, lax.rem(peer, GROUP)], got4.at[i, q], s4.at[i], r4.at[i],
                device_id=peer, device_id_type=FLAT
            ).start()

        each_peer(GROUP, send4)
        got4[i, q] = snd4[i, q]

    for s in range(2):
        wait_bytes(pack.at[s, pl.ds(0, GROUP - 1)], s1.at[s])
        wait_bytes(rcv.at[s, pl.ds(0, 2 * (ALL - 1))], s2.at[s])
        wait_bytes(back1.at[s, pl.ds(0, ALL - 1)], s31.at[s])
    wait_bytes(back0.at[pl.ds(0, ALL - 1)], s30)
    for i in range(2):
        wait_bytes(got4.at[i, pl.ds(0, GROUP - 1)], r4.at[i])

        def unpack(p, carry):
            value = got4[i, p]
            out_ref[2 * p + i, 0:16] = value[:, :64]
            out_ref[2 * p + i, 16:32] = value[:, 64:]
            return carry

        lax.fori_loop(0, GROUP, unpack, 0, unroll=4)
    for i in range(2):
        wait_bytes(snd4.at[i, pl.ds(0, GROUP - 1)], s4.at[i])


def per_device(source, green):
    lines, forward, inverse = tables()
    vmem = pltpu.VMEM
    dma = pltpu.SemaphoreType.DMA
    result = pl.pallas_call(
        kernel,
        out_shape=jax.ShapeDtypeStruct((64, 32, 64), F32),
        in_specs=[pl.BlockSpec(memory_space=pl.ANY)] * 5,
        out_specs=pl.BlockSpec(memory_space=vmem),
        scratch_shapes=[
            vmem((64, 32, 64), F32),
            vmem((2, GROUP, 16, 128), F32),
            vmem((6, 256, 256), BF16),
            vmem((2, 256, 512), BF16),
            vmem((2, 256, 512), BF16),
            vmem((2, GROUP, 16, 128), F32),
            vmem((256, 256), F32),
            vmem((256, 512), F32),
            vmem((2, 2, ALL, 8, 128), F32),
            vmem((2, 256, 8, 128), F32),
            vmem((ALL, 2, 8, 128), F32),
            vmem((2, ALL, 8, 128), F32),
            vmem((512, 16, 128), F32),
            vmem((2, 8, 512, 128), F32),
            vmem((2, 512, 128), F32),
            vmem((2, GROUP, 16, 128), F32),
            vmem((2, GROUP, 16, 128), F32),
            dma, dma((3,)), dma, dma((2,)), dma((2,)), dma((2,)), dma((2,)),
            dma, dma, dma((2,)), dma((2,)), dma((2,)), dma((2,)),
        ],
        compiler_params=pltpu.CompilerParams(
            collective_id=1, has_side_effects=True, vmem_limit_bytes=56 * 2**20
        ),
        name="poisson",
    )(jnp.transpose(source, (0, 2, 1)), green,
      jnp.asarray(lines), jnp.asarray(forward), jnp.asarray(inverse))
    return jnp.transpose(result, (0, 2, 1))


def solution(mesh):
    return jax.shard_map(
        per_device,
        mesh=mesh,
        in_specs=(P("gx", "gy", "gz"), P(None, ("gx", "gz"), "gy")),
        out_specs=P("gx", "gy", "gz"),
        check_vma=False,
    )
```

```python
import jax
import jax.numpy as jnp
import numpy as np
from jax import lax
from jax.experimental import pallas as pl
from jax.experimental.pallas import tpu as pltpu
from jax.sharding import PartitionSpec as P

FLAT = pl.DeviceIdType.LOGICAL
F32 = jnp.float32
BF16 = jnp.bfloat16
GX, GY, GZ = 4, 4, 8
GROUP = GY * GZ
ALL = GX * GROUP


def halves(table):
    high = np.asarray(table, np.float32).astype(BF16)
    low = (np.asarray(table) - high.astype(np.float64)).astype(np.float32).astype(BF16)
    return np.stack([high, low])


def tables():
    n = np.arange(256)
    angle = 2.0 * np.pi * ((n[:, None] * n[None, :]) % 512) / 512.0
    parity = 1.0 - 2.0 * (n % 2)
    cos, sin = np.cos(angle), np.sin(angle)
    sin_rows = sin.copy()
    sin_rows[0, :] = parity
    sin_cols = sin.copy()
    sin_cols[:, 0] = parity
    lines = np.concatenate([halves(cos), halves(sin_rows), halves(sin_cols)])
    real = cos.reshape(256, 4, 1, 64)
    imag = -sin
    imag[:, 0] = parity
    forward = np.concatenate([real, imag.reshape(256, 4, 1, 64)], axis=2)
    weight = np.full((4, 2, 64), 2.0)
    weight[0, :, 0] = 1.0
    inverse = (forward * weight[None]).reshape(256, 512)
    return lines, halves(forward.reshape(256, 512)), halves(inverse)


def split(value):
    high = value.astype(BF16)
    return high, (value - high.astype(F32)).astype(BF16)


def dot(left, right):
    return jnp.dot(left, right, preferred_element_type=F32)


def dot_t(left, right):
    return lax.dot_general(left, right, (((1,), (1,)), ((), ())), preferred_element_type=F32)


def dot3(left, right):
    return dot(left[0], right[0]) + (dot(left[1], right[0]) + dot(left[0], right[1]))


def wide(left, right):
    return jnp.concatenate([left, right], axis=1)


def kernel(src_hbm, green_hbm, lines_hbm, zf_hbm, zi_hbm, out_ref,
           src, pack, lines, zf, zi, got1, zs, zb, snd, rcv, back0, back1, gbuf, gs, gmix, snd4, got4,
           in_sem, tab_sem, green_sem, s1, r1, s2, r2, s30, r30, s31, r31, s4, r4):
    a, b, c = lax.axis_index("gx"), lax.axis_index("gy"), lax.axis_index("gz")
    q = b * GZ + c
    me = a * GROUP + q

    load_src = pltpu.make_async_copy(src_hbm, src, in_sem)
    load_src.start()
    loads = [pltpu.make_async_copy(lines_hbm, lines, tab_sem.at[0]),
             pltpu.make_async_copy(zf_hbm, zf, tab_sem.at[1]),
             pltpu.make_async_copy(zi_hbm, zi, tab_sem.at[2])]
    for load in loads:
        load.start()

    def wait_bytes(part, sem):
        pltpu.make_async_copy(part, part, sem).wait()

    def hops(o):
        ring = (0, 1, 2, 1)
        return ring[o & 3] + 2 * ((o >> 2) & 1) + ring[(o >> 3) & 3]

    far_first = sorted(range(1, GROUP), key=hops, reverse=True)

    def each_peer(count, body):
        if count == GROUP:
            for o in far_first:
                body(lax.bitwise_xor(me, o))
            return

        def step(o, carry):
            body(lax.bitwise_xor(me, lax.rem(o * 19, count)))
            return carry

        lax.fori_loop(1, count, step, 0, unroll=8)

    bar = pltpu.get_barrier_semaphore()

    def greet(peer):
        pl.semaphore_signal(bar, inc=1, device_id=peer, device_id_type=FLAT)

    each_peer(GROUP, greet)
    for o in range(1, GX):
        greet(lax.bitwise_xor(me, o * GROUP))
    load_src.wait()

    def pack_x(p, carry):
        for i in range(2):
            plane = src[2 * p + i]
            pack[i, p] = wide(plane[:16], plane[16:])
        return carry

    lax.fori_loop(0, GROUP, pack_x, 0, unroll=4)
    pl.semaphore_wait(bar, GROUP - 1 + GX - 1)

    for i in range(2):
        def send1(peer):
            pltpu.make_async_remote_copy(
                pack.at[i, lax.rem(peer, GROUP)], got1.at[i, q], s1.at[i], r1.at[i],
                device_id=peer, device_id_type=FLAT
            ).start()

        each_peer(GROUP, send1)
        got1[i, q] = pack[i, q]

    pltpu.make_async_copy(green_hbm.at[pl.ds(0, 257)], gbuf.at[pl.ds(0, 257)], green_sem).start()

    def load_green(k, carry):
        pltpu.make_async_copy(green_hbm.at[512 - k], gbuf.at[256 + k], green_sem).start()
        return carry

    lax.fori_loop(1, 256, load_green, 0, unroll=5)
    for load in loads:
        load.wait()

    low_lane = lax.broadcasted_iota(jnp.int32, (1, 128), 1) < 64
    sign = jnp.where(low_lane, 1.0, -1.0).astype(F32)
    real_lane = lax.broadcasted_iota(jnp.int32, (1, 128), 1) == 0
    imag_lane = lax.broadcasted_iota(jnp.int32, (1, 128), 1) == 64
    unit_lane = jnp.logical_or(real_lane, imag_lane)
    top_row = lax.broadcasted_iota(jnp.int32, (8, 1), 0) == 0

    def half_turn(value):
        return pltpu.roll(value, 64, 1)

    def turn(value):
        return sign * half_turn(value)

    def fix_top(value, top):
        return jnp.concatenate([jnp.where(top_row, top, value[:8]), value[8:]], axis=0)

    cos = (lines[0], lines[1])
    sin_rows = (lines[2], lines[3])
    sin_cols = (lines[4], lines[5])
    snd_view = snd.reshape(2, 2, GX, GY, GZ, 8, 128)

    def send2(s, i):
        def send(peer):
            pltpu.make_async_remote_copy(
                snd.at[s, i, peer], rcv.at[s, 2 * me + i], s2.at[s], r2.at[s],
                device_id=peer, device_id_type=FLAT
            ).start()

        each_peer(ALL, send)
        rcv[s, 2 * me + i] = snd[s, i, me]

    for i in range(2):
        wait_bytes(got1.at[i, pl.ds(0, GROUP - 1)], r1.at[i])

        def gather(t, carry):
            for th in range(2):
                left = got1[i, 2 * th * GZ + t]
                right = got1[i, (2 * th + 1) * GZ + t]
                row = pl.multiple_of(t * 32, 32)
                zs[pl.ds(row, 16), th * 128:(th + 1) * 128] = jnp.where(low_lane, left, half_turn(right))
                zs[pl.ds(row + 16, 16), th * 128:(th + 1) * 128] = jnp.where(low_lane, half_turn(left), right)
            return carry

        lax.fori_loop(0, GZ, gather, 0, unroll=2)
        zb[...] = dot3(split(jnp.transpose(zs[...])), (zf[0], zf[1]))

        def forward_y(t, carry):
            column = pl.multiple_of(t * 256, 256)
            value = zb[:, pl.ds(column, 256)]
            even = dot3(cos, split(value))
            odd = dot3(sin_rows, split(wide(turn(value[:, :128]), turn(value[:, 128:]))))
            for h in range(2):
                ev, od = even[:, h * 128:(h + 1) * 128], odd[:, h * 128:(h + 1) * 128]
                plus, minus = ev + od, ev - od
                if h == 0:
                    special = jnp.logical_and(unit_lane, t == 0)
                    plus = jnp.where(special, jnp.where(real_lane, ev, od), plus)
                    minus = jnp.where(special, jnp.where(real_lane, half_turn(ev), -half_turn(od)), minus)
                plus = fix_top(plus, ev[:8])
                minus = fix_top(minus, -turn(od[:8]))
                snd_view[0, i, :, 2 * t + h] = plus.reshape(GX, GZ, 8, 128)
                snd_view[1, i, :, 2 * t + h] = minus.reshape(GX, GZ, 8, 128)
            return carry

        lax.fori_loop(0, GY // 2, forward_y, 0)
        send2(0, i)
    for i in range(2):
        send2(1, i)

    pltpu.make_async_copy(green_hbm, gbuf, green_sem).wait()
    green_rows = gbuf.reshape(512 * 16, 128)
    corner = jnp.logical_and(b == 0, jnp.logical_and(a == 0, c == 0))
    pick = 2 * lax.rem(lax.broadcasted_iota(jnp.int32, (512, 128), 1), 64)

    def prepare(jj, carry):
        first = green_rows[pl.ds(2 * jj, 512, stride=16), :]
        second = green_rows[pl.ds(2 * jj + 1, 512, stride=16), :]
        here = jnp.logical_and(corner, jj == 0)
        plus = jnp.take_along_axis(first, pick, axis=1)
        minus = jnp.take_along_axis(second, pick, axis=1)
        first0, first1 = first[:, 0:1], first[:, 1:2]
        second0, second1 = second[:, 0:1], second[:, 1:2]
        at_unit = jnp.logical_and(unit_lane, b == 0)
        plus_unit = jnp.where(here, 0.5 * (first0 + first1), first0)
        minus_unit = jnp.where(here, 0.5 * (second0 + second1), first1)
        gs[0, jj] = jnp.where(at_unit, plus_unit, plus)
        gs[1, jj] = jnp.where(at_unit, minus_unit, minus)

        @pl.when(jj == 0)
        def _():
            gmix[0] = jnp.where(jnp.logical_and(unit_lane, here), 0.5 * (first0 - first1), 0.0)
            gmix[1] = jnp.where(jnp.logical_and(unit_lane, here), 0.5 * (second0 - second1), 0.0)

        return carry

    lax.fori_loop(0, 8, prepare, 0)

    rcv_rows = rcv.reshape(2 * 256 * 8, 128)
    for s in range(2):
        wait_bytes(rcv.at[s, pl.ds(0, 2 * (ALL - 1))], r2.at[s])

        def lines_x(jp, carry):
            first = pl.ds(s * 2048 + 2 * jp, 256, stride=8)
            second = pl.ds(s * 2048 + 2 * jp + 1, 256, stride=8)
            left, right = rcv_rows[first, :], rcv_rows[second, :]
            even = dot3(cos, split(wide(left, right)))
            odd = dot3(sin_rows, split(wide(turn(left), turn(right))))
            results = []
            for h in range(2):
                ev, od = even[:, h * 128:(h + 1) * 128], odd[:, h * 128:(h + 1) * 128]
                plus = fix_top(ev + od, ev[:8])
                minus = fix_top(ev - od, -turn(od[:8]))
                out_plus = plus * gs[s, 2 * jp + h, 0:256]
                out_minus = minus * gs[s, 2 * jp + h, 256:512]
                if h == 0:
                    mix = jnp.where(jp == 0, 1.0, 0.0) * sign
                    out_plus += gmix[s, 0:256] * (mix * fix_top(minus, plus[:8]))
                    out_minus += gmix[s, 256:512] * (mix * fix_top(plus, minus[:8]))
                total = fix_top(out_plus + out_minus, out_plus[:8])
                turned = fix_top(turn(out_plus - out_minus), -out_minus[:8])
                results.append((total, turned))
            total = wide(results[0][0], results[1][0])
            turned = wide(results[0][1], results[1][1])
            back_x = dot3(cos, split(total)) - dot3(sin_cols, split(turned))
            rcv_rows[first, :] = back_x[:, :128]
            rcv_rows[second, :] = back_x[:, 128:]
            return carry

        lax.fori_loop(0, 4, lines_x, 0)

        if s == 0:
            def send30(peer):
                pltpu.make_async_remote_copy(
                    rcv.at[0, pl.ds(2 * peer, 2)], back0.at[me], s30, r30,
                    device_id=peer, device_id_type=FLAT
                ).start()

            each_peer(ALL, send30)
            back0[me] = rcv[0, pl.ds(2 * me, 2)]
        else:
            for i in range(2):
                def send31(peer):
                    pltpu.make_async_remote_copy(
                        rcv.at[1, 2 * peer + i], back1.at[i, me], s31.at[i], r31.at[i],
                        device_id=peer, device_id_type=FLAT
                    ).start()

                each_peer(ALL, send31)
                back1[i, me] = rcv[1, 2 * me + i]

    back0_view = back0.reshape(GX, GY, GZ, 2, 8, 128)
    back1_view = back1.reshape(2, GX, GY, GZ, 8, 128)
    wait_bytes(back0.at[pl.ds(0, ALL - 1)], r30)
    for i in range(2):
        wait_bytes(back1.at[i, pl.ds(0, ALL - 1)], r31.at[i])

        def inverse_y(t, carry):
            totals, turneds = [], []
            for h in range(2):
                plus = back0_view[:, 2 * t + h, :, i].reshape(256, 128)
                minus = back1_view[i, :, 2 * t + h].reshape(256, 128)
                total = plus + minus
                turned = turn(plus - minus)
                if h == 0:
                    special = jnp.logical_and(unit_lane, t == 0)
                    total = jnp.where(special, 2.0 * jnp.where(real_lane, plus, half_turn(minus)), total)
                    turned = jnp.where(special, 2.0 * jnp.where(real_lane, half_turn(plus), minus), turned)
                totals.append(fix_top(total, plus[:8]))
                turneds.append(fix_top(turned, -minus[:8]))
            column = pl.multiple_of(t * 256, 256)
            zb[:, pl.ds(column, 256)] = (
                dot3(cos, split(wide(*totals))) - dot3(sin_cols, split(wide(*turneds)))
            )
            return carry

        lax.fori_loop(0, GY // 2, inverse_y, 0)
        high, low = split(zb[...])
        zs[...] = (dot_t(zi[0], high) + (dot_t(zi[1], high) + dot_t(zi[0], low))) * (1.0 / 134217728.0)

        def scatter(t, carry):
            row = pl.multiple_of(t * 32, 32)
            for th in range(2):
                upper = zs[pl.ds(row, 16), th * 128:(th + 1) * 128]
                lower = zs[pl.ds(row + 16, 16), th * 128:(th + 1) * 128]
                snd4[i, 2 * th * GZ + t] = jnp.where(low_lane, upper, half_turn(lower))
                snd4[i, (2 * th + 1) * GZ + t] = jnp.where(low_lane, half_turn(upper), lower)
            return carry

        lax.fori_loop(0, GZ, scatter, 0, unroll=2)

        def send4(peer):
            pltpu.make_async_remote_copy(
                snd4.at[i, lax.rem(peer, GROUP)], got4.at[i, q], s4.at[i], r4.at[i],
                device_id=peer, device_id_type=FLAT
            ).start()

        each_peer(GROUP, send4)
        got4[i, q] = snd4[i, q]

    for s in range(2):
        wait_bytes(pack.at[s, pl.ds(0, GROUP - 1)], s1.at[s])
        wait_bytes(rcv.at[s, pl.ds(0, 2 * (ALL - 1))], s2.at[s])
        wait_bytes(back1.at[s, pl.ds(0, ALL - 1)], s31.at[s])
    wait_bytes(back0.at[pl.ds(0, ALL - 1)], s30)
    for i in range(2):
        wait_bytes(got4.at[i, pl.ds(0, GROUP - 1)], r4.at[i])

        def unpack(p, carry):
            value = got4[i, p]
            out_ref[2 * p + i, 0:16] = value[:, :64]
            out_ref[2 * p + i, 16:32] = value[:, 64:]
            return carry

        lax.fori_loop(0, GROUP, unpack, 0, unroll=4)
    for i in range(2):
        wait_bytes(snd4.at[i, pl.ds(0, GROUP - 1)], s4.at[i])


def per_device(source, green):
    lines, forward, inverse = tables()
    vmem = pltpu.VMEM
    dma = pltpu.SemaphoreType.DMA
    result = pl.pallas_call(
        kernel,
        out_shape=jax.ShapeDtypeStruct((64, 32, 64), F32),
        in_specs=[pl.BlockSpec(memory_space=pl.ANY)] * 5,
        out_specs=pl.BlockSpec(memory_space=vmem),
        scratch_shapes=[
            vmem((64, 32, 64), F32),
            vmem((2, GROUP, 16, 128), F32),
            vmem((6, 256, 256), BF16),
            vmem((2, 256, 512), BF16),
            vmem((2, 256, 512), BF16),
            vmem((2, GROUP, 16, 128), F32),
            vmem((256, 256), F32),
            vmem((256, 512), F32),
            vmem((2, 2, ALL, 8, 128), F32),
            vmem((2, 256, 8, 128), F32),
            vmem((ALL, 2, 8, 128), F32),
            vmem((2, ALL, 8, 128), F32),
            vmem((512, 16, 128), F32),
            vmem((2, 8, 512, 128), F32),
            vmem((2, 512, 128), F32),
            vmem((2, GROUP, 16, 128), F32),
            vmem((2, GROUP, 16, 128), F32),
            dma, dma((3,)), dma, dma((2,)), dma((2,)), dma((2,)), dma((2,)),
            dma, dma, dma((2,)), dma((2,)), dma((2,)), dma((2,)),
        ],
        compiler_params=pltpu.CompilerParams(
            collective_id=1, has_side_effects=True, vmem_limit_bytes=34 * 2**20
        ),
        name="poisson",
    )(*[pltpu.with_memory_space_constraint(v, pltpu.HBM) for v in (
        jnp.transpose(source, (0, 2, 1)), green,
        jnp.asarray(lines), jnp.asarray(forward), jnp.asarray(inverse))])
    return jnp.transpose(result, (0, 2, 1))


def solution(mesh):
    return jax.shard_map(
        per_device,
        mesh=mesh,
        in_specs=(P("gx", "gy", "gz"), P(None, ("gx", "gz"), "gy")),
        out_specs=P("gx", "gy", "gz"),
        check_vma=False,
    )
```

```python
import jax
import jax.numpy as jnp
import numpy as np
from jax import lax
from jax.experimental import pallas as pl
from jax.experimental.pallas import tpu as pltpu
from jax.sharding import PartitionSpec as P

FLAT = pl.DeviceIdType.LOGICAL
F32 = jnp.float32
BF16 = jnp.bfloat16
GX, GY, GZ = 4, 4, 8
GROUP = GY * GZ
ALL = GX * GROUP


def halves(table):
    high = np.asarray(table, np.float32).astype(BF16)
    low = (np.asarray(table) - high.astype(np.float64)).astype(np.float32).astype(BF16)
    return np.stack([high, low])


def tables():
    n = np.arange(256)
    angle = 2.0 * np.pi * ((n[:, None] * n[None, :]) % 512) / 512.0
    parity = 1.0 - 2.0 * (n % 2)
    cos, sin = np.cos(angle), np.sin(angle)
    sin_rows = sin.copy()
    sin_rows[0, :] = parity
    sin_cols = sin.copy()
    sin_cols[:, 0] = parity
    lines = np.concatenate([halves(cos), halves(sin_rows), halves(sin_cols)])
    real = cos.reshape(256, 4, 1, 64)
    imag = -sin
    imag[:, 0] = parity
    forward = np.concatenate([real, imag.reshape(256, 4, 1, 64)], axis=2)
    weight = np.full((4, 2, 64), 2.0)
    weight[0, :, 0] = 1.0
    inverse = (forward * weight[None]).reshape(256, 512)
    return lines, halves(forward.reshape(256, 512)), halves(inverse)


def split(value):
    high = value.astype(BF16)
    return high, (value - high.astype(F32)).astype(BF16)


def dot(left, right):
    return jnp.dot(left, right, preferred_element_type=F32)


def dot_t(left, right):
    return lax.dot_general(left, right, (((1,), (1,)), ((), ())), preferred_element_type=F32)


def dot3(left, right):
    return dot(left[0], right[0]) + (dot(left[1], right[0]) + dot(left[0], right[1]))


def wide(left, right):
    return jnp.concatenate([left, right], axis=1)


def kernel(src_hbm, green_hbm, lines_hbm, zf_hbm, zi_hbm, out_ref,
           src, pack, lines, zf, zi, got1, zs, zb, snd, rcv, back0, back1, gbuf, gs, gmix, snd4, got4,
           in_sem, tab_sem, green_sem, s1, r1, s2, r2, s30, r30, s31, r31, s4, r4):
    a, b, c = lax.axis_index("gx"), lax.axis_index("gy"), lax.axis_index("gz")
    q = b * GZ + c
    me = a * GROUP + q

    load_src = pltpu.make_async_copy(src_hbm, src, in_sem)
    load_src.start()
    loads = [pltpu.make_async_copy(lines_hbm, lines, tab_sem.at[0]),
             pltpu.make_async_copy(zf_hbm, zf, tab_sem.at[1]),
             pltpu.make_async_copy(zi_hbm, zi, tab_sem.at[2])]
    for load in loads:
        load.start()

    def wait_bytes(part, sem):
        pltpu.make_async_copy(part, part, sem).wait()

    def hops(o):
        ring = (0, 1, 2, 1)
        return ring[o & 3] + 2 * ((o >> 2) & 1) + ring[(o >> 3) & 3]

    far_first = sorted(range(1, GROUP), key=hops, reverse=True)

    def each_peer(count, body):
        if count == GROUP:
            for o in far_first:
                body(lax.bitwise_xor(me, o))
            return

        def step(o, carry):
            body(lax.bitwise_xor(me, lax.rem(o * 19, count)))
            return carry

        lax.fori_loop(1, count, step, 0, unroll=8)

    bar = pltpu.get_barrier_semaphore()

    def greet(peer):
        pl.semaphore_signal(bar, inc=1, device_id=peer, device_id_type=FLAT)

    each_peer(GROUP, greet)
    for o in range(1, GX):
        greet(lax.bitwise_xor(me, o * GROUP))
    load_src.wait()

    def pack_x(p, carry):
        for i in range(2):
            plane = src[2 * p + i]
            pack[i, p] = wide(plane[:16], plane[16:])
        return carry

    lax.fori_loop(0, GROUP, pack_x, 0, unroll=4)
    pl.semaphore_wait(bar, GROUP - 1 + GX - 1)

    for i in range(2):
        def send1(peer):
            pltpu.make_async_remote_copy(
                pack.at[i, lax.rem(peer, GROUP)], got1.at[i, q], s1.at[i], r1.at[i],
                device_id=peer, device_id_type=FLAT
            ).start()

        each_peer(GROUP, send1)
        got1[i, q] = pack[i, q]

    pltpu.make_async_copy(green_hbm.at[pl.ds(0, 257)], gbuf.at[pl.ds(0, 257)], green_sem).start()

    def load_green(k, carry):
        pltpu.make_async_copy(green_hbm.at[512 - k], gbuf.at[256 + k], green_sem).start()
        return carry

    lax.fori_loop(1, 256, load_green, 0, unroll=5)
    for load in loads:
        load.wait()

    low_lane = lax.broadcasted_iota(jnp.int32, (1, 128), 1) < 64
    sign = jnp.where(low_lane, 1.0, -1.0).astype(F32)
    real_lane = lax.broadcasted_iota(jnp.int32, (1, 128), 1) == 0
    imag_lane = lax.broadcasted_iota(jnp.int32, (1, 128), 1) == 64
    unit_lane = jnp.logical_or(real_lane, imag_lane)
    top_row = lax.broadcasted_iota(jnp.int32, (8, 1), 0) == 0

    def half_turn(value):
        return pltpu.roll(value, 64, 1)

    def turn(value):
        return sign * half_turn(value)

    def fix_top(value, top):
        return jnp.concatenate([jnp.where(top_row, top, value[:8]), value[8:]], axis=0)

    cos = (lines[0], lines[1])
    sin_rows = (lines[2], lines[3])
    sin_cols = (lines[4], lines[5])
    snd_view = snd.reshape(2, 2, GX, GY, GZ, 8, 128)

    def send2(s, i):
        def send(peer):
            pltpu.make_async_remote_copy(
                snd.at[s, i, peer], rcv.at[s, 2 * me + i], s2.at[s], r2.at[s],
                device_id=peer, device_id_type=FLAT
            ).start()

        each_peer(ALL, send)
        rcv[s, 2 * me + i] = snd[s, i, me]

    for i in range(2):
        wait_bytes(got1.at[i, pl.ds(0, GROUP - 1)], r1.at[i])

        def gather(t, carry):
            for th in range(2):
                left = got1[i, 2 * th * GZ + t]
                right = got1[i, (2 * th + 1) * GZ + t]
                row = pl.multiple_of(t * 32, 32)
                zs[pl.ds(row, 16), th * 128:(th + 1) * 128] = jnp.where(low_lane, left, half_turn(right))
                zs[pl.ds(row + 16, 16), th * 128:(th + 1) * 128] = jnp.where(low_lane, half_turn(left), right)
            return carry

        lax.fori_loop(0, GZ, gather, 0, unroll=True)
        zb[...] = dot3(split(jnp.transpose(zs[...])), (zf[0], zf[1]))

        def forward_y(t, carry):
            column = pl.multiple_of(t * 256, 256)
            value = zb[:, pl.ds(column, 256)]
            even = dot3(cos, split(value))
            odd = dot3(sin_rows, split(wide(turn(value[:, :128]), turn(value[:, 128:]))))
            for h in range(2):
                ev, od = even[:, h * 128:(h + 1) * 128], odd[:, h * 128:(h + 1) * 128]
                plus, minus = ev + od, ev - od
                if h == 0:
                    special = jnp.logical_and(unit_lane, t == 0)
                    plus = jnp.where(special, jnp.where(real_lane, ev, od), plus)
                    minus = jnp.where(special, jnp.where(real_lane, half_turn(ev), -half_turn(od)), minus)
                plus = fix_top(plus, ev[:8])
                minus = fix_top(minus, -turn(od[:8]))
                snd_view[0, i, :, 2 * t + h] = plus.reshape(GX, GZ, 8, 128)
                snd_view[1, i, :, 2 * t + h] = minus.reshape(GX, GZ, 8, 128)
            return carry

        lax.fori_loop(0, GY // 2, forward_y, 0, unroll=True)
        send2(0, i)
    for i in range(2):
        send2(1, i)

    pltpu.make_async_copy(green_hbm, gbuf, green_sem).wait()
    green_rows = gbuf.reshape(512 * 16, 128)
    corner = jnp.logical_and(b == 0, jnp.logical_and(a == 0, c == 0))
    pick = 2 * lax.rem(lax.broadcasted_iota(jnp.int32, (512, 128), 1), 64)

    def prepare(jj, carry):
        first = green_rows[pl.ds(2 * jj, 512, stride=16), :]
        second = green_rows[pl.ds(2 * jj + 1, 512, stride=16), :]
        here = jnp.logical_and(corner, jj == 0)
        plus = jnp.take_along_axis(first, pick, axis=1)
        minus = jnp.take_along_axis(second, pick, axis=1)
        first0, first1 = first[:, 0:1], first[:, 1:2]
        second0, second1 = second[:, 0:1], second[:, 1:2]
        at_unit = jnp.logical_and(unit_lane, b == 0)
        plus_unit = jnp.where(here, 0.5 * (first0 + first1), first0)
        minus_unit = jnp.where(here, 0.5 * (second0 + second1), first1)
        gs[0, jj] = jnp.where(at_unit, plus_unit, plus)
        gs[1, jj] = jnp.where(at_unit, minus_unit, minus)

        @pl.when(jj == 0)
        def _():
            gmix[0] = jnp.where(jnp.logical_and(unit_lane, here), 0.5 * (first0 - first1), 0.0)
            gmix[1] = jnp.where(jnp.logical_and(unit_lane, here), 0.5 * (second0 - second1), 0.0)

        return carry

    lax.fori_loop(0, 8, prepare, 0)

    rcv_rows = rcv.reshape(2 * 256 * 8, 128)
    for s in range(2):
        wait_bytes(rcv.at[s, pl.ds(0, 2 * (ALL - 1))], r2.at[s])

        def lines_x(jp, carry):
            first = pl.ds(s * 2048 + 2 * jp, 256, stride=8)
            second = pl.ds(s * 2048 + 2 * jp + 1, 256, stride=8)
            left, right = rcv_rows[first, :], rcv_rows[second, :]
            even = dot3(cos, split(wide(left, right)))
            odd = dot3(sin_rows, split(wide(turn(left), turn(right))))
            results = []
            for h in range(2):
                ev, od = even[:, h * 128:(h + 1) * 128], odd[:, h * 128:(h + 1) * 128]
                plus = fix_top(ev + od, ev[:8])
                minus = fix_top(ev - od, -turn(od[:8]))
                out_plus = plus * gs[s, 2 * jp + h, 0:256]
                out_minus = minus * gs[s, 2 * jp + h, 256:512]
                if h == 0:
                    mix = jnp.where(jp == 0, 1.0, 0.0) * sign
                    out_plus += gmix[s, 0:256] * (mix * fix_top(minus, plus[:8]))
                    out_minus += gmix[s, 256:512] * (mix * fix_top(plus, minus[:8]))
                total = fix_top(out_plus + out_minus, out_plus[:8])
                turned = fix_top(turn(out_plus - out_minus), -out_minus[:8])
                results.append((total, turned))
            total = wide(results[0][0], results[1][0])
            turned = wide(results[0][1], results[1][1])
            back_x = dot3(cos, split(total)) - dot3(sin_cols, split(turned))
            rcv_rows[first, :] = back_x[:, :128]
            rcv_rows[second, :] = back_x[:, 128:]
            return carry

        lax.fori_loop(0, 4, lines_x, 0)

        if s == 0:
            def send30(peer):
                pltpu.make_async_remote_copy(
                    rcv.at[0, pl.ds(2 * peer, 2)], back0.at[me], s30, r30,
                    device_id=peer, device_id_type=FLAT
                ).start()

            each_peer(ALL, send30)
            back0[me] = rcv[0, pl.ds(2 * me, 2)]
        else:
            for i in range(2):
                def send31(peer):
                    pltpu.make_async_remote_copy(
                        rcv.at[1, 2 * peer + i], back1.at[i, me], s31.at[i], r31.at[i],
                        device_id=peer, device_id_type=FLAT
                    ).start()

                each_peer(ALL, send31)
                back1[i, me] = rcv[1, 2 * me + i]

    back0_view = back0.reshape(GX, GY, GZ, 2, 8, 128)
    back1_view = back1.reshape(2, GX, GY, GZ, 8, 128)
    wait_bytes(back0.at[pl.ds(0, ALL - 1)], r30)
    for i in range(2):
        wait_bytes(back1.at[i, pl.ds(0, ALL - 1)], r31.at[i])

        def inverse_y(t, carry):
            totals, turneds = [], []
            for h in range(2):
                plus = back0_view[:, 2 * t + h, :, i].reshape(256, 128)
                minus = back1_view[i, :, 2 * t + h].reshape(256, 128)
                total = plus + minus
                turned = turn(plus - minus)
                if h == 0:
                    special = jnp.logical_and(unit_lane, t == 0)
                    total = jnp.where(special, 2.0 * jnp.where(real_lane, plus, half_turn(minus)), total)
                    turned = jnp.where(special, 2.0 * jnp.where(real_lane, half_turn(plus), minus), turned)
                totals.append(fix_top(total, plus[:8]))
                turneds.append(fix_top(turned, -minus[:8]))
            column = pl.multiple_of(t * 256, 256)
            zb[:, pl.ds(column, 256)] = (
                dot3(cos, split(wide(*totals))) - dot3(sin_cols, split(wide(*turneds)))
            )
            return carry

        lax.fori_loop(0, GY // 2, inverse_y, 0, unroll=True)
        high, low = split(zb[...])
        zs[...] = (dot_t(zi[0], high) + (dot_t(zi[1], high) + dot_t(zi[0], low))) * (1.0 / 134217728.0)

        def scatter(t, carry):
            row = pl.multiple_of(t * 32, 32)
            for th in range(2):
                upper = zs[pl.ds(row, 16), th * 128:(th + 1) * 128]
                lower = zs[pl.ds(row + 16, 16), th * 128:(th + 1) * 128]
                snd4[i, 2 * th * GZ + t] = jnp.where(low_lane, upper, half_turn(lower))
                snd4[i, (2 * th + 1) * GZ + t] = jnp.where(low_lane, half_turn(upper), lower)
            return carry

        lax.fori_loop(0, GZ, scatter, 0, unroll=True)

        def send4(peer):
            pltpu.make_async_remote_copy(
                snd4.at[i, lax.rem(peer, GROUP)], got4.at[i, q], s4.at[i], r4.at[i],
                device_id=peer, device_id_type=FLAT
            ).start()

        each_peer(GROUP, send4)
        got4[i, q] = snd4[i, q]

    for s in range(2):
        wait_bytes(pack.at[s, pl.ds(0, GROUP - 1)], s1.at[s])
        wait_bytes(rcv.at[s, pl.ds(0, 2 * (ALL - 1))], s2.at[s])
        wait_bytes(back1.at[s, pl.ds(0, ALL - 1)], s31.at[s])
    wait_bytes(back0.at[pl.ds(0, ALL - 1)], s30)
    for i in range(2):
        wait_bytes(got4.at[i, pl.ds(0, GROUP - 1)], r4.at[i])

        def unpack(p, carry):
            value = got4[i, p]
            out_ref[2 * p + i, 0:16] = value[:, :64]
            out_ref[2 * p + i, 16:32] = value[:, 64:]
            return carry

        lax.fori_loop(0, GROUP, unpack, 0, unroll=4)
    for i in range(2):
        wait_bytes(snd4.at[i, pl.ds(0, GROUP - 1)], s4.at[i])


def per_device(source, green):
    lines, forward, inverse = tables()
    vmem = pltpu.VMEM
    dma = pltpu.SemaphoreType.DMA
    result = pl.pallas_call(
        kernel,
        out_shape=jax.ShapeDtypeStruct((64, 32, 64), F32),
        in_specs=[pl.BlockSpec(memory_space=pl.ANY)] * 5,
        out_specs=pl.BlockSpec(memory_space=vmem),
        scratch_shapes=[
            vmem((64, 32, 64), F32),
            vmem((2, GROUP, 16, 128), F32),
            vmem((6, 256, 256), BF16),
            vmem((2, 256, 512), BF16),
            vmem((2, 256, 512), BF16),
            vmem((2, GROUP, 16, 128), F32),
            vmem((256, 256), F32),
            vmem((256, 512), F32),
            vmem((2, 2, ALL, 8, 128), F32),
            vmem((2, 256, 8, 128), F32),
            vmem((ALL, 2, 8, 128), F32),
            vmem((2, ALL, 8, 128), F32),
            vmem((512, 16, 128), F32),
            vmem((2, 8, 512, 128), F32),
            vmem((2, 512, 128), F32),
            vmem((2, GROUP, 16, 128), F32),
            vmem((2, GROUP, 16, 128), F32),
            dma, dma((3,)), dma, dma((2,)), dma((2,)), dma((2,)), dma((2,)),
            dma, dma, dma((2,)), dma((2,)), dma((2,)), dma((2,)),
        ],
        compiler_params=pltpu.CompilerParams(
            collective_id=1, has_side_effects=True, vmem_limit_bytes=34 * 2**20
        ),
        name="poisson",
    )(*[pltpu.with_memory_space_constraint(v, pltpu.HBM) for v in (
        jnp.transpose(source, (0, 2, 1)), green,
        jnp.asarray(lines), jnp.asarray(forward), jnp.asarray(inverse))])
    return jnp.transpose(result, (0, 2, 1))


def solution(mesh):
    return jax.shard_map(
        per_device,
        mesh=mesh,
        in_specs=(P("gx", "gy", "gz"), P(None, ("gx", "gz"), "gy")),
        out_specs=P("gx", "gy", "gz"),
        check_vma=False,
    )
```

```python
import jax
import jax.numpy as jnp
import numpy as np
from jax import lax
from jax.experimental import pallas as pl
from jax.experimental.pallas import tpu as pltpu
from jax.sharding import PartitionSpec as P

FLAT = pl.DeviceIdType.LOGICAL
F32 = jnp.float32
BF16 = jnp.bfloat16
GX, GY, GZ = 4, 4, 8
GROUP = GY * GZ
ALL = GX * GROUP


def halves(table):
    high = np.asarray(table, np.float32).astype(BF16)
    low = (np.asarray(table) - high.astype(np.float64)).astype(np.float32).astype(BF16)
    return np.stack([high, low])


def tables():
    n = np.arange(256)
    angle = 2.0 * np.pi * ((n[:, None] * n[None, :]) % 512) / 512.0
    parity = 1.0 - 2.0 * (n % 2)
    cos, sin = np.cos(angle), np.sin(angle)
    sin_rows = sin.copy()
    sin_rows[0, :] = parity
    sin_cols = sin.copy()
    sin_cols[:, 0] = parity
    lines = np.concatenate([halves(cos), halves(sin_rows), halves(sin_cols)])
    real = cos.reshape(256, 4, 1, 64)
    imag = -sin
    imag[:, 0] = parity
    forward = np.concatenate([real, imag.reshape(256, 4, 1, 64)], axis=2)
    weight = np.full((4, 2, 64), 2.0)
    weight[0, :, 0] = 1.0
    inverse = (forward * weight[None]).reshape(256, 512)
    return lines, halves(forward.reshape(256, 512)), halves(inverse)


def split(value):
    high = value.astype(BF16)
    return high, (value - high.astype(F32)).astype(BF16)


def dot(left, right):
    return jnp.dot(left, right, preferred_element_type=F32)


def dot_t(left, right):
    return lax.dot_general(left, right, (((1,), (1,)), ((), ())), preferred_element_type=F32)


def dot3(left, right):
    return dot(left[0], right[0]) + (dot(left[1], right[0]) + dot(left[0], right[1]))


def wide(left, right):
    return jnp.concatenate([left, right], axis=1)


def kernel(src_hbm, green_hbm, lines_hbm, zf_hbm, zi_hbm, out_ref,
           src, pack, lines, zf, zi, got1, zs, zb, snd, rcv, back0, back1, gbuf, gs, gmix, snd4, got4,
           in_sem, tab_sem, green_sem, s1, r1, s2, r2, s30, r30, s31, r31, s4, r4):
    a, b, c = lax.axis_index("gx"), lax.axis_index("gy"), lax.axis_index("gz")
    q = b * GZ + c
    me = a * GROUP + q

    load_src = [pltpu.make_async_copy(src_hbm.at[:, i], src.at[i], in_sem.at[i]) for i in range(2)]
    for load in load_src:
        load.start()
    loads = [pltpu.make_async_copy(lines_hbm, lines, tab_sem.at[0]),
             pltpu.make_async_copy(zf_hbm, zf, tab_sem.at[1]),
             pltpu.make_async_copy(zi_hbm, zi, tab_sem.at[2])]
    for load in loads:
        load.start()

    def wait_bytes(part, sem):
        pltpu.make_async_copy(part, part, sem).wait()

    def hops(o):
        ring = (0, 1, 2, 1)
        return ring[o & 3] + 2 * ((o >> 2) & 1) + ring[(o >> 3) & 3]

    far_first = sorted(range(1, GROUP), key=hops, reverse=True)

    def each_peer(count, body):
        if count == GROUP:
            for o in far_first:
                body(lax.bitwise_xor(me, o))
            return

        def step(o, carry):
            body(lax.bitwise_xor(me, lax.rem(o * 19, count)))
            return carry

        lax.fori_loop(1, count, step, 0, unroll=8)

    bar = pltpu.get_barrier_semaphore()

    def greet(peer):
        pl.semaphore_signal(bar, inc=1, device_id=peer, device_id_type=FLAT)

    each_peer(GROUP, greet)
    for o in range(1, GX):
        greet(lax.bitwise_xor(me, o * GROUP))

    def pack_plane(i):
        load_src[i].wait()

        def pack_x(p, carry):
            plane = src[i, p]
            pack[i, p] = wide(plane[:16], plane[16:])
            return carry

        lax.fori_loop(0, GROUP, pack_x, 0, unroll=8)

    pack_plane(0)
    pl.semaphore_wait(bar, GROUP - 1 + GX - 1)

    for i in range(2):
        def send1(peer):
            pltpu.make_async_remote_copy(
                pack.at[i, lax.rem(peer, GROUP)], got1.at[i, q], s1.at[i], r1.at[i],
                device_id=peer, device_id_type=FLAT
            ).start()

        each_peer(GROUP, send1)
        got1[i, q] = pack[i, q]
        if i == 0:
            pack_plane(1)

    pltpu.make_async_copy(green_hbm.at[pl.ds(0, 257)], gbuf.at[pl.ds(0, 257)], green_sem).start()

    def load_green(k, carry):
        pltpu.make_async_copy(green_hbm.at[512 - k], gbuf.at[256 + k], green_sem).start()
        return carry

    lax.fori_loop(1, 256, load_green, 0, unroll=5)
    for load in loads:
        load.wait()

    low_lane = lax.broadcasted_iota(jnp.int32, (1, 128), 1) < 64
    sign = jnp.where(low_lane, 1.0, -1.0).astype(F32)
    real_lane = lax.broadcasted_iota(jnp.int32, (1, 128), 1) == 0
    imag_lane = lax.broadcasted_iota(jnp.int32, (1, 128), 1) == 64
    unit_lane = jnp.logical_or(real_lane, imag_lane)
    top_row = lax.broadcasted_iota(jnp.int32, (8, 1), 0) == 0

    def half_turn(value):
        return pltpu.roll(value, 64, 1)

    def turn(value):
        return sign * half_turn(value)

    def fix_top(value, top):
        return jnp.concatenate([jnp.where(top_row, top, value[:8]), value[8:]], axis=0)

    cos = (lines[0], lines[1])
    sin_rows = (lines[2], lines[3])
    sin_cols = (lines[4], lines[5])
    snd_view = snd.reshape(2, 2, GX, GY, GZ, 8, 128)

    def send2(s, i):
        def send(peer):
            pltpu.make_async_remote_copy(
                snd.at[s, i, peer], rcv.at[s, 2 * me + i], s2.at[s], r2.at[s],
                device_id=peer, device_id_type=FLAT
            ).start()

        each_peer(ALL, send)
        rcv[s, 2 * me + i] = snd[s, i, me]

    for i in range(2):
        wait_bytes(got1.at[i, pl.ds(0, GROUP - 1)], r1.at[i])

        def gather(t, carry):
            for th in range(2):
                left = got1[i, 2 * th * GZ + t]
                right = got1[i, (2 * th + 1) * GZ + t]
                row = pl.multiple_of(t * 32, 32)
                zs[pl.ds(row, 16), th * 128:(th + 1) * 128] = jnp.where(low_lane, left, half_turn(right))
                zs[pl.ds(row + 16, 16), th * 128:(th + 1) * 128] = jnp.where(low_lane, half_turn(left), right)
            return carry

        lax.fori_loop(0, GZ, gather, 0, unroll=True)
        zb[...] = dot3(split(jnp.transpose(zs[...])), (zf[0], zf[1]))

        def forward_y(t, carry):
            column = pl.multiple_of(t * 256, 256)
            value = zb[:, pl.ds(column, 256)]
            even = dot3(cos, split(value))
            odd = dot3(sin_rows, split(wide(turn(value[:, :128]), turn(value[:, 128:]))))
            for h in range(2):
                ev, od = even[:, h * 128:(h + 1) * 128], odd[:, h * 128:(h + 1) * 128]
                plus, minus = ev + od, ev - od
                if h == 0:
                    special = jnp.logical_and(unit_lane, t == 0)
                    plus = jnp.where(special, jnp.where(real_lane, ev, od), plus)
                    minus = jnp.where(special, jnp.where(real_lane, half_turn(ev), -half_turn(od)), minus)
                plus = fix_top(plus, ev[:8])
                minus = fix_top(minus, -turn(od[:8]))
                snd_view[0, i, :, 2 * t + h] = plus.reshape(GX, GZ, 8, 128)
                snd_view[1, i, :, 2 * t + h] = minus.reshape(GX, GZ, 8, 128)
            return carry

        lax.fori_loop(0, GY // 2, forward_y, 0, unroll=True)
        send2(0, i)
    for i in range(2):
        send2(1, i)

    pltpu.make_async_copy(green_hbm, gbuf, green_sem).wait()
    green_rows = gbuf.reshape(512 * 16, 128)
    corner = jnp.logical_and(b == 0, jnp.logical_and(a == 0, c == 0))
    pick = 2 * lax.rem(lax.broadcasted_iota(jnp.int32, (512, 128), 1), 64)

    def prepare(jj, carry):
        first = green_rows[pl.ds(2 * jj, 512, stride=16), :]
        second = green_rows[pl.ds(2 * jj + 1, 512, stride=16), :]
        here = jnp.logical_and(corner, jj == 0)
        plus = jnp.take_along_axis(first, pick, axis=1)
        minus = jnp.take_along_axis(second, pick, axis=1)
        first0, first1 = first[:, 0:1], first[:, 1:2]
        second0, second1 = second[:, 0:1], second[:, 1:2]
        at_unit = jnp.logical_and(unit_lane, b == 0)
        plus_unit = jnp.where(here, 0.5 * (first0 + first1), first0)
        minus_unit = jnp.where(here, 0.5 * (second0 + second1), first1)
        gs[0, jj] = jnp.where(at_unit, plus_unit, plus)
        gs[1, jj] = jnp.where(at_unit, minus_unit, minus)

        @pl.when(jj == 0)
        def _():
            gmix[0] = jnp.where(jnp.logical_and(unit_lane, here), 0.5 * (first0 - first1), 0.0)
            gmix[1] = jnp.where(jnp.logical_and(unit_lane, here), 0.5 * (second0 - second1), 0.0)

        return carry

    lax.fori_loop(0, 8, prepare, 0)

    rcv_rows = rcv.reshape(2 * 256 * 8, 128)
    for s in range(2):
        wait_bytes(rcv.at[s, pl.ds(0, 2 * (ALL - 1))], r2.at[s])

        def lines_x(jp, carry):
            first = pl.ds(s * 2048 + 2 * jp, 256, stride=8)
            second = pl.ds(s * 2048 + 2 * jp + 1, 256, stride=8)
            left, right = rcv_rows[first, :], rcv_rows[second, :]
            even = dot3(cos, split(wide(left, right)))
            odd = dot3(sin_rows, split(wide(turn(left), turn(right))))
            results = []
            for h in range(2):
                ev, od = even[:, h * 128:(h + 1) * 128], odd[:, h * 128:(h + 1) * 128]
                plus = fix_top(ev + od, ev[:8])
                minus = fix_top(ev - od, -turn(od[:8]))
                out_plus = plus * gs[s, 2 * jp + h, 0:256]
                out_minus = minus * gs[s, 2 * jp + h, 256:512]
                if h == 0:
                    mix = jnp.where(jp == 0, 1.0, 0.0) * sign
                    out_plus += gmix[s, 0:256] * (mix * fix_top(minus, plus[:8]))
                    out_minus += gmix[s, 256:512] * (mix * fix_top(plus, minus[:8]))
                total = fix_top(out_plus + out_minus, out_plus[:8])
                turned = fix_top(turn(out_plus - out_minus), -out_minus[:8])
                results.append((total, turned))
            total = wide(results[0][0], results[1][0])
            turned = wide(results[0][1], results[1][1])
            back_x = dot3(cos, split(total)) - dot3(sin_cols, split(turned))
            rcv_rows[first, :] = back_x[:, :128]
            rcv_rows[second, :] = back_x[:, 128:]
            return carry

        lax.fori_loop(0, 4, lines_x, 0)

        if s == 0:
            def send30(peer):
                pltpu.make_async_remote_copy(
                    rcv.at[0, pl.ds(2 * peer, 2)], back0.at[me], s30, r30,
                    device_id=peer, device_id_type=FLAT
                ).start()

            each_peer(ALL, send30)
            back0[me] = rcv[0, pl.ds(2 * me, 2)]
        else:
            for i in range(2):
                def send31(peer):
                    pltpu.make_async_remote_copy(
                        rcv.at[1, 2 * peer + i], back1.at[i, me], s31.at[i], r31.at[i],
                        device_id=peer, device_id_type=FLAT
                    ).start()

                each_peer(ALL, send31)
                back1[i, me] = rcv[1, 2 * me + i]

    back0_view = back0.reshape(GX, GY, GZ, 2, 8, 128)
    back1_view = back1.reshape(2, GX, GY, GZ, 8, 128)
    wait_bytes(back0.at[pl.ds(0, ALL - 1)], r30)
    for i in range(2):
        wait_bytes(back1.at[i, pl.ds(0, ALL - 1)], r31.at[i])

        def inverse_y(t, carry):
            totals, turneds = [], []
            for h in range(2):
                plus = back0_view[:, 2 * t + h, :, i].reshape(256, 128)
                minus = back1_view[i, :, 2 * t + h].reshape(256, 128)
                total = plus + minus
                turned = turn(plus - minus)
                if h == 0:
                    special = jnp.logical_and(unit_lane, t == 0)
                    total = jnp.where(special, 2.0 * jnp.where(real_lane, plus, half_turn(minus)), total)
                    turned = jnp.where(special, 2.0 * jnp.where(real_lane, half_turn(plus), minus), turned)
                totals.append(fix_top(total, plus[:8]))
                turneds.append(fix_top(turned, -minus[:8]))
            column = pl.multiple_of(t * 256, 256)
            zb[:, pl.ds(column, 256)] = (
                dot3(cos, split(wide(*totals))) - dot3(sin_cols, split(wide(*turneds)))
            )
            return carry

        lax.fori_loop(0, GY // 2, inverse_y, 0, unroll=True)
        high, low = split(zb[...])
        zs[...] = (dot_t(zi[0], high) + (dot_t(zi[1], high) + dot_t(zi[0], low))) * (1.0 / 134217728.0)

        def scatter(t, carry):
            row = pl.multiple_of(t * 32, 32)
            for th in range(2):
                upper = zs[pl.ds(row, 16), th * 128:(th + 1) * 128]
                lower = zs[pl.ds(row + 16, 16), th * 128:(th + 1) * 128]
                snd4[i, 2 * th * GZ + t] = jnp.where(low_lane, upper, half_turn(lower))
                snd4[i, (2 * th + 1) * GZ + t] = jnp.where(low_lane, half_turn(upper), lower)
            return carry

        lax.fori_loop(0, GZ, scatter, 0, unroll=True)

        def send4(peer):
            pltpu.make_async_remote_copy(
                snd4.at[i, lax.rem(peer, GROUP)], got4.at[i, q], s4.at[i], r4.at[i],
                device_id=peer, device_id_type=FLAT
            ).start()

        each_peer(GROUP, send4)
        got4[i, q] = snd4[i, q]

    for s in range(2):
        wait_bytes(pack.at[s, pl.ds(0, GROUP - 1)], s1.at[s])
        wait_bytes(rcv.at[s, pl.ds(0, 2 * (ALL - 1))], s2.at[s])
        wait_bytes(back1.at[s, pl.ds(0, ALL - 1)], s31.at[s])
    wait_bytes(back0.at[pl.ds(0, ALL - 1)], s30)
    for i in range(2):
        wait_bytes(got4.at[i, pl.ds(0, GROUP - 1)], r4.at[i])

        def unpack(p, carry):
            value = got4[i, p]
            out_ref[2 * p + i, 0:16] = value[:, :64]
            out_ref[2 * p + i, 16:32] = value[:, 64:]
            return carry

        lax.fori_loop(0, GROUP, unpack, 0, unroll=4)
    for i in range(2):
        wait_bytes(snd4.at[i, pl.ds(0, GROUP - 1)], s4.at[i])


def per_device(source, green):
    lines, forward, inverse = tables()
    vmem = pltpu.VMEM
    dma = pltpu.SemaphoreType.DMA
    result = pl.pallas_call(
        kernel,
        out_shape=jax.ShapeDtypeStruct((64, 32, 64), F32),
        in_specs=[pl.BlockSpec(memory_space=pl.ANY)] * 5,
        out_specs=pl.BlockSpec(memory_space=vmem),
        scratch_shapes=[
            vmem((2, GROUP, 32, 64), F32),
            vmem((2, GROUP, 16, 128), F32),
            vmem((6, 256, 256), BF16),
            vmem((2, 256, 512), BF16),
            vmem((2, 256, 512), BF16),
            vmem((2, GROUP, 16, 128), F32),
            vmem((256, 256), F32),
            vmem((256, 512), F32),
            vmem((2, 2, ALL, 8, 128), F32),
            vmem((2, 256, 8, 128), F32),
            vmem((ALL, 2, 8, 128), F32),
            vmem((2, ALL, 8, 128), F32),
            vmem((512, 16, 128), F32),
            vmem((2, 8, 512, 128), F32),
            vmem((2, 512, 128), F32),
            vmem((2, GROUP, 16, 128), F32),
            vmem((2, GROUP, 16, 128), F32),
            dma((2,)), dma((3,)), dma, dma((2,)), dma((2,)), dma((2,)), dma((2,)),
            dma, dma, dma((2,)), dma((2,)), dma((2,)), dma((2,)),
        ],
        compiler_params=pltpu.CompilerParams(
            collective_id=1, has_side_effects=True, vmem_limit_bytes=34 * 2**20
        ),
        name="poisson",
    )(*[pltpu.with_memory_space_constraint(v, pltpu.HBM) for v in (
        jnp.transpose(source, (0, 2, 1)).reshape(GROUP, 2, 32, 64), green,
        jnp.asarray(lines), jnp.asarray(forward), jnp.asarray(inverse))])
    return jnp.transpose(result, (0, 2, 1))


def solution(mesh):
    return jax.shard_map(
        per_device,
        mesh=mesh,
        in_specs=(P("gx", "gy", "gz"), P(None, ("gx", "gz"), "gy")),
        out_specs=P("gx", "gy", "gz"),
        check_vma=False,
    )
```

```python
import jax
import jax.numpy as jnp
import numpy as np
from jax import lax
from jax.experimental import pallas as pl
from jax.experimental.pallas import tpu as pltpu
from jax.sharding import PartitionSpec as P

FLAT = pl.DeviceIdType.LOGICAL
F32 = jnp.float32
BF16 = jnp.bfloat16
GX, GY, GZ = 4, 4, 8
GROUP = GY * GZ
ALL = GX * GROUP


def halves(table):
    high = np.asarray(table, np.float32).astype(BF16)
    low = (np.asarray(table) - high.astype(np.float64)).astype(np.float32).astype(BF16)
    return np.stack([high, low])


def tables():
    n = np.arange(256)
    angle = 2.0 * np.pi * ((n[:, None] * n[None, :]) % 512) / 512.0
    parity = 1.0 - 2.0 * (n % 2)
    cos, sin = np.cos(angle), np.sin(angle)
    sin_rows = sin.copy()
    sin_rows[0, :] = parity
    sin_cols = sin.copy()
    sin_cols[:, 0] = parity
    lines = np.concatenate([halves(cos), halves(sin_rows), halves(sin_cols)])
    real = cos.reshape(256, 4, 1, 64)
    imag = -sin
    imag[:, 0] = parity
    forward = np.concatenate([real, imag.reshape(256, 4, 1, 64)], axis=2)
    weight = np.full((4, 2, 64), 2.0)
    weight[0, :, 0] = 1.0
    inverse = (forward * weight[None]).reshape(256, 512)
    return lines, halves(forward.reshape(256, 512)), halves(inverse)


def split(value):
    high = value.astype(BF16)
    return high, (value - high.astype(F32)).astype(BF16)


def dot(left, right):
    return jnp.dot(left, right, preferred_element_type=F32)


def dot_t(left, right):
    return lax.dot_general(left, right, (((1,), (1,)), ((), ())), preferred_element_type=F32)


def dot3(left, right):
    return dot(left[0], right[0]) + (dot(left[1], right[0]) + dot(left[0], right[1]))


def wide(left, right):
    return jnp.concatenate([left, right], axis=1)


def kernel(src_hbm, green_hbm, lines_hbm, zf_hbm, zi_hbm, out_ref,
           src, pack, lines, zf, zi, got1, zs, zb, snd, rcv, back0, back1, gbuf, gs, gmix, snd4, got4,
           in_sem, tab_sem, green_sem, s1, r1, s2, r2, s30, r30, s31, r31, s4, r4):
    a, b, c = lax.axis_index("gx"), lax.axis_index("gy"), lax.axis_index("gz")
    q = b * GZ + c
    me = a * GROUP + q

    load_src = [pltpu.make_async_copy(src_hbm.at[:, i], src.at[i], in_sem.at[i]) for i in range(2)]
    for load in load_src:
        load.start()
    loads = [pltpu.make_async_copy(lines_hbm, lines, tab_sem.at[0]),
             pltpu.make_async_copy(zf_hbm, zf, tab_sem.at[1]),
             pltpu.make_async_copy(zi_hbm, zi, tab_sem.at[2])]
    for load in loads:
        load.start()

    def wait_bytes(part, sem):
        pltpu.make_async_copy(part, part, sem).wait()

    def hops(o):
        ring = (0, 1, 2, 1)
        return ring[o & 3] + 2 * ((o >> 2) & 1) + ring[(o >> 3) & 3]

    far_first = sorted(range(1, GROUP), key=hops, reverse=True)

    def each_peer(count, body, factor=19):
        if count == GROUP:
            for o in far_first:
                body(lax.bitwise_xor(me, o))
            return

        def step(o, carry):
            body(lax.bitwise_xor(me, lax.rem(o * factor, count)))
            return carry

        lax.fori_loop(1, count, step, 0, unroll=8)

    bar = pltpu.get_barrier_semaphore()

    def greet(peer):
        pl.semaphore_signal(bar, inc=1, device_id=peer, device_id_type=FLAT)

    each_peer(GROUP, greet)
    for o in range(1, GX):
        greet(lax.bitwise_xor(me, o * GROUP))

    def pack_plane(i):
        load_src[i].wait()

        def pack_x(p, carry):
            plane = src[i, p]
            pack[i, p] = wide(plane[:16], plane[16:])
            return carry

        lax.fori_loop(0, GROUP, pack_x, 0, unroll=8)

    pack_plane(0)
    pl.semaphore_wait(bar, GROUP - 1 + GX - 1)

    for i in range(2):
        def send1(peer):
            pltpu.make_async_remote_copy(
                pack.at[i, lax.rem(peer, GROUP)], got1.at[i, q], s1.at[i], r1.at[i],
                device_id=peer, device_id_type=FLAT
            ).start()

        each_peer(GROUP, send1)
        got1[i, q] = pack[i, q]
        if i == 0:
            pack_plane(1)

    pltpu.make_async_copy(green_hbm.at[pl.ds(0, 257)], gbuf.at[pl.ds(0, 257)], green_sem).start()

    def load_green(k, carry):
        pltpu.make_async_copy(green_hbm.at[512 - k], gbuf.at[256 + k], green_sem).start()
        return carry

    lax.fori_loop(1, 256, load_green, 0, unroll=5)
    for load in loads:
        load.wait()

    low_lane = lax.broadcasted_iota(jnp.int32, (1, 128), 1) < 64
    sign = jnp.where(low_lane, 1.0, -1.0).astype(F32)
    real_lane = lax.broadcasted_iota(jnp.int32, (1, 128), 1) == 0
    imag_lane = lax.broadcasted_iota(jnp.int32, (1, 128), 1) == 64
    unit_lane = jnp.logical_or(real_lane, imag_lane)
    top_row = lax.broadcasted_iota(jnp.int32, (8, 1), 0) == 0

    def half_turn(value):
        return pltpu.roll(value, 64, 1)

    def turn(value):
        return sign * half_turn(value)

    def fix_top(value, top):
        return jnp.concatenate([jnp.where(top_row, top, value[:8]), value[8:]], axis=0)

    cos = (lines[0], lines[1])
    sin_rows = (lines[2], lines[3])
    sin_cols = (lines[4], lines[5])
    snd_view = snd.reshape(2, 2, GX, GY, GZ, 8, 128)

    def send2(s, i):
        def send(peer):
            pltpu.make_async_remote_copy(
                snd.at[s, i, peer], rcv.at[s, 2 * me + i], s2.at[s], r2.at[s],
                device_id=peer, device_id_type=FLAT
            ).start()

        each_peer(ALL, send)
        rcv[s, 2 * me + i] = snd[s, i, me]

    for i in range(2):
        wait_bytes(got1.at[i, pl.ds(0, GROUP - 1)], r1.at[i])

        def gather(t, carry):
            for th in range(2):
                left = got1[i, 2 * th * GZ + t]
                right = got1[i, (2 * th + 1) * GZ + t]
                row = pl.multiple_of(t * 32, 32)
                zs[pl.ds(row, 16), th * 128:(th + 1) * 128] = jnp.where(low_lane, left, half_turn(right))
                zs[pl.ds(row + 16, 16), th * 128:(th + 1) * 128] = jnp.where(low_lane, half_turn(left), right)
            return carry

        lax.fori_loop(0, GZ, gather, 0, unroll=True)
        zb[...] = dot3(split(jnp.transpose(zs[...])), (zf[0], zf[1]))

        def forward_y(t, carry):
            column = pl.multiple_of(t * 256, 256)
            value = zb[:, pl.ds(column, 256)]
            even = dot3(cos, split(value))
            odd = dot3(sin_rows, split(wide(turn(value[:, :128]), turn(value[:, 128:]))))
            for h in range(2):
                ev, od = even[:, h * 128:(h + 1) * 128], odd[:, h * 128:(h + 1) * 128]
                plus, minus = ev + od, ev - od
                if h == 0:
                    special = jnp.logical_and(unit_lane, t == 0)
                    plus = jnp.where(special, jnp.where(real_lane, ev, od), plus)
                    minus = jnp.where(special, jnp.where(real_lane, half_turn(ev), -half_turn(od)), minus)
                plus = fix_top(plus, ev[:8])
                minus = fix_top(minus, -turn(od[:8]))
                snd_view[0, i, :, 2 * t + h] = plus.reshape(GX, GZ, 8, 128)
                snd_view[1, i, :, 2 * t + h] = minus.reshape(GX, GZ, 8, 128)
            return carry

        lax.fori_loop(0, GY // 2, forward_y, 0, unroll=True)
        send2(0, i)
    for i in range(2):
        send2(1, i)

    pltpu.make_async_copy(green_hbm, gbuf, green_sem).wait()
    green_rows = gbuf.reshape(512 * 16, 128)
    corner = jnp.logical_and(b == 0, jnp.logical_and(a == 0, c == 0))
    pick = 2 * lax.rem(lax.broadcasted_iota(jnp.int32, (512, 128), 1), 64)

    def prepare(jj, carry):
        first = green_rows[pl.ds(2 * jj, 512, stride=16), :]
        second = green_rows[pl.ds(2 * jj + 1, 512, stride=16), :]
        here = jnp.logical_and(corner, jj == 0)
        plus = jnp.take_along_axis(first, pick, axis=1)
        minus = jnp.take_along_axis(second, pick, axis=1)
        first0, first1 = first[:, 0:1], first[:, 1:2]
        second0, second1 = second[:, 0:1], second[:, 1:2]
        at_unit = jnp.logical_and(unit_lane, b == 0)
        plus_unit = jnp.where(here, 0.5 * (first0 + first1), first0)
        minus_unit = jnp.where(here, 0.5 * (second0 + second1), first1)
        gs[0, jj] = jnp.where(at_unit, plus_unit, plus)
        gs[1, jj] = jnp.where(at_unit, minus_unit, minus)

        @pl.when(jj == 0)
        def _():
            gmix[0] = jnp.where(jnp.logical_and(unit_lane, here), 0.5 * (first0 - first1), 0.0)
            gmix[1] = jnp.where(jnp.logical_and(unit_lane, here), 0.5 * (second0 - second1), 0.0)

        return carry

    lax.fori_loop(0, 8, prepare, 0)

    rcv_rows = rcv.reshape(2 * 256 * 8, 128)
    for s in range(2):
        wait_bytes(rcv.at[s, pl.ds(0, 2 * (ALL - 1))], r2.at[s])

        def lines_x(jp, carry):
            first = pl.ds(s * 2048 + 2 * jp, 256, stride=8)
            second = pl.ds(s * 2048 + 2 * jp + 1, 256, stride=8)
            left, right = rcv_rows[first, :], rcv_rows[second, :]
            even = dot3(cos, split(wide(left, right)))
            odd = dot3(sin_rows, split(wide(turn(left), turn(right))))
            results = []
            for h in range(2):
                ev, od = even[:, h * 128:(h + 1) * 128], odd[:, h * 128:(h + 1) * 128]
                plus = fix_top(ev + od, ev[:8])
                minus = fix_top(ev - od, -turn(od[:8]))
                out_plus = plus * gs[s, 2 * jp + h, 0:256]
                out_minus = minus * gs[s, 2 * jp + h, 256:512]
                if h == 0:
                    mix = jnp.where(jp == 0, 1.0, 0.0) * sign
                    out_plus += gmix[s, 0:256] * (mix * fix_top(minus, plus[:8]))
                    out_minus += gmix[s, 256:512] * (mix * fix_top(plus, minus[:8]))
                total = fix_top(out_plus + out_minus, out_plus[:8])
                turned = fix_top(turn(out_plus - out_minus), -out_minus[:8])
                results.append((total, turned))
            total = wide(results[0][0], results[1][0])
            turned = wide(results[0][1], results[1][1])
            back_x = dot3(cos, split(total)) - dot3(sin_cols, split(turned))
            rcv_rows[first, :] = back_x[:, :128]
            rcv_rows[second, :] = back_x[:, 128:]
            return carry

        lax.fori_loop(0, 4, lines_x, 0)

        if s == 0:
            def send30(peer):
                pltpu.make_async_remote_copy(
                    rcv.at[0, pl.ds(2 * peer, 2)], back0.at[me], s30, r30,
                    device_id=peer, device_id_type=FLAT
                ).start()

            each_peer(ALL, send30, 83)
            back0[me] = rcv[0, pl.ds(2 * me, 2)]
        else:
            for i in range(2):
                def send31(peer):
                    pltpu.make_async_remote_copy(
                        rcv.at[1, 2 * peer + i], back1.at[i, me], s31.at[i], r31.at[i],
                        device_id=peer, device_id_type=FLAT
                    ).start()

                each_peer(ALL, send31, 83)
                back1[i, me] = rcv[1, 2 * me + i]

    back0_view = back0.reshape(GX, GY, GZ, 2, 8, 128)
    back1_view = back1.reshape(2, GX, GY, GZ, 8, 128)
    wait_bytes(back0.at[pl.ds(0, ALL - 1)], r30)
    for i in range(2):
        wait_bytes(back1.at[i, pl.ds(0, ALL - 1)], r31.at[i])

        def inverse_y(t, carry):
            totals, turneds = [], []
            for h in range(2):
                plus = back0_view[:, 2 * t + h, :, i].reshape(256, 128)
                minus = back1_view[i, :, 2 * t + h].reshape(256, 128)
                total = plus + minus
                turned = turn(plus - minus)
                if h == 0:
                    special = jnp.logical_and(unit_lane, t == 0)
                    total = jnp.where(special, 2.0 * jnp.where(real_lane, plus, half_turn(minus)), total)
                    turned = jnp.where(special, 2.0 * jnp.where(real_lane, half_turn(plus), minus), turned)
                totals.append(fix_top(total, plus[:8]))
                turneds.append(fix_top(turned, -minus[:8]))
            column = pl.multiple_of(t * 256, 256)
            zb[:, pl.ds(column, 256)] = (
                dot3(cos, split(wide(*totals))) - dot3(sin_cols, split(wide(*turneds)))
            )
            return carry

        lax.fori_loop(0, GY // 2, inverse_y, 0, unroll=True)
        high, low = split(zb[...])
        zs[...] = (dot_t(zi[0], high) + (dot_t(zi[1], high) + dot_t(zi[0], low))) * (1.0 / 134217728.0)

        def scatter(t, carry):
            row = pl.multiple_of(t * 32, 32)
            for th in range(2):
                upper = zs[pl.ds(row, 16), th * 128:(th + 1) * 128]
                lower = zs[pl.ds(row + 16, 16), th * 128:(th + 1) * 128]
                snd4[i, 2 * th * GZ + t] = jnp.where(low_lane, upper, half_turn(lower))
                snd4[i, (2 * th + 1) * GZ + t] = jnp.where(low_lane, half_turn(upper), lower)
            return carry

        lax.fori_loop(0, GZ, scatter, 0, unroll=True)

        def send4(peer):
            pltpu.make_async_remote_copy(
                snd4.at[i, lax.rem(peer, GROUP)], got4.at[i, q], s4.at[i], r4.at[i],
                device_id=peer, device_id_type=FLAT
            ).start()

        each_peer(GROUP, send4)
        got4[i, q] = snd4[i, q]

    for s in range(2):
        wait_bytes(pack.at[s, pl.ds(0, GROUP - 1)], s1.at[s])
        wait_bytes(rcv.at[s, pl.ds(0, 2 * (ALL - 1))], s2.at[s])
        wait_bytes(back1.at[s, pl.ds(0, ALL - 1)], s31.at[s])
    wait_bytes(back0.at[pl.ds(0, ALL - 1)], s30)
    for i in range(2):
        wait_bytes(got4.at[i, pl.ds(0, GROUP - 1)], r4.at[i])

        def unpack(p, carry):
            value = got4[i, p]
            out_ref[2 * p + i, 0:16] = value[:, :64]
            out_ref[2 * p + i, 16:32] = value[:, 64:]
            return carry

        lax.fori_loop(0, GROUP, unpack, 0, unroll=4)
    for i in range(2):
        wait_bytes(snd4.at[i, pl.ds(0, GROUP - 1)], s4.at[i])


def per_device(source, green):
    lines, forward, inverse = tables()
    vmem = pltpu.VMEM
    dma = pltpu.SemaphoreType.DMA
    result = pl.pallas_call(
        kernel,
        out_shape=jax.ShapeDtypeStruct((64, 32, 64), F32),
        in_specs=[pl.BlockSpec(memory_space=pl.ANY)] * 5,
        out_specs=pl.BlockSpec(memory_space=vmem),
        scratch_shapes=[
            vmem((2, GROUP, 32, 64), F32),
            vmem((2, GROUP, 16, 128), F32),
            vmem((6, 256, 256), BF16),
            vmem((2, 256, 512), BF16),
            vmem((2, 256, 512), BF16),
            vmem((2, GROUP, 16, 128), F32),
            vmem((256, 256), F32),
            vmem((256, 512), F32),
            vmem((2, 2, ALL, 8, 128), F32),
            vmem((2, 256, 8, 128), F32),
            vmem((ALL, 2, 8, 128), F32),
            vmem((2, ALL, 8, 128), F32),
            vmem((512, 16, 128), F32),
            vmem((2, 8, 512, 128), F32),
            vmem((2, 512, 128), F32),
            vmem((2, GROUP, 16, 128), F32),
            vmem((2, GROUP, 16, 128), F32),
            dma((2,)), dma((3,)), dma, dma((2,)), dma((2,)), dma((2,)), dma((2,)),
            dma, dma, dma((2,)), dma((2,)), dma((2,)), dma((2,)),
        ],
        compiler_params=pltpu.CompilerParams(
            collective_id=1, has_side_effects=True, vmem_limit_bytes=34 * 2**20
        ),
        name="poisson",
    )(*[pltpu.with_memory_space_constraint(v, pltpu.HBM) for v in (
        jnp.transpose(source, (0, 2, 1)).reshape(GROUP, 2, 32, 64), green,
        jnp.asarray(lines), jnp.asarray(forward), jnp.asarray(inverse))])
    return jnp.transpose(result, (0, 2, 1))


def solution(mesh):
    return jax.shard_map(
        per_device,
        mesh=mesh,
        in_specs=(P("gx", "gy", "gz"), P(None, ("gx", "gz"), "gy")),
        out_specs=P("gx", "gy", "gz"),
        check_vma=False,
    )
```
